32 devices in a mesh: seq: 16 (over z, y, x), rep: 2 (over core).
Axes of the slice: x: 2, y: 2, z: 4, core: 2. Of those that a mesh axis runs over, the one named last changes fastest.
Arguments:
- queries: bfloat16 [4096, 4096], P(('rep', 'seq')), parts along dimension 0, may hold values from -160 to 160
- keys_values: bfloat16 [2, 4096, 1024], P(None, ('rep', 'seq')), parts along dimension 1, may hold values from -6 to 6
- segment_ids: int32 [4096], P(('rep', 'seq')), parts along dimension 0, may hold values from 0 to 31, never falling along the last dimension, each value on 1 to 1024 neighbouring positions
Outputs:
- attended: bfloat16 [4096, 4096], P(('rep', 'seq')), parts along dimension 0
The draws below stay inside these ranges and needn't reach their ends.
There are 2 independent parts, one for each index of `rep`. The reference program is written for one: setup_inputs(seed, part) draws one part's arguments, and reference() takes and returns one part's arrays. A program takes and returns all parts, laid end to end along the dimension named above; each array names one. Nothing has to cross between parts.
Inputs may be any that keep to these rules, and one draw needn't show every extreme that they name: `segment_ids`: ids never fall along the tokens; every document holds 1 to 1024 consecutive tokens, one exactly 1024.
All inputs are finite; a program needn't handle non-finite values.
Results may differ from the reference program's by a relative error of at most 0.004.
Values may be sent and summed in bfloat16 or wider, within the bound.
No kernel may reach another device: no remote copies, remote signals or barrier semaphores. Data moves between devices by JAX's collectives and lax.ppermute only.
A program may use at most 192 MiB of HBM per device.

```python
import math
import jax
import jax.numpy as jnp
import numpy as np
from jax import lax

HQ = 32
HK = 8
DH = 128
WINDOW = 2048
DOC_COUNT = 32
TOKENS = 2048
DOC_MOST = 1024


def shared_draw(key):
    shape_keys = (TOKENS, HK * DH)
    key_rows = jnp.clip(jax.random.normal(jax.random.fold_in(key, 101), shape_keys, jnp.float32), -6.0, 6.0)
    value_rows = jnp.clip(jax.random.normal(jax.random.fold_in(key, 102), shape_keys, jnp.float32), -6.0, 6.0)
    query_rows = jnp.clip(jax.random.normal(jax.random.fold_in(key, 103), (TOKENS, HQ * DH), jnp.float32), -6.0, 6.0)
    return (query_rows, jnp.stack([key_rows, value_rows]))


def draw_queries(key, part):
    return shared_draw(key)[0].astype(jnp.bfloat16)


def draw_keys_values(key, part):
    return shared_draw(key)[1].astype(jnp.bfloat16)


def length_profile(amount, total, limit, slope):
    weights = [(1 << 20) // math.isqrt(standing ** slope) + 1 for standing in range(2, amount + 1)]
    spare, given = total - limit - (amount - 1), [1] * (amount - 1)
    while spare > 0:
        free = [i for i in range(amount - 1) if given[i] < limit]
        whole, budget = sum([weights[i] for i in free]), spare
        for i in free:
            addition = min(limit - given[i], max(1, budget * weights[i] // whole), spare)
            given[i] = given[i] + addition
            spare = spare - addition
    return np.array([limit] + given)


def uneven_parts(own_key, number_of, total, limit, skew):
    if number_of == 2:
        one = jax.random.randint(own_key, (), max(1, total - limit), min(limit, total - 1) + 1)
        return jnp.stack([one, total - one])
    tallies = jnp.asarray(length_profile(number_of, total, limit, skew), jnp.int32)
    couples = (number_of - 1) // 2
    donor, receiver = tallies[1:1 + 2 * couples:2], tallies[2:2 + 2 * couples:2]
    room = jnp.minimum(donor - 1, limit - receiver)
    moved = jax.random.randint(jax.random.fold_in(own_key, 1), (couples,), 0, 1 << 20) % (room + 1)
    tallies = tallies.at[1:1 + 2 * couples:2].set(donor - moved).at[2:2 + 2 * couples:2].set(receiver + moved)
    return tallies[jax.random.permutation(jax.random.fold_in(own_key, 2), number_of)]


def setup_inputs(seed: int = 0, part: int = 0) -> dict:
    streams_of = jax.random.split(jax.random.key(seed), 4)
    part_keys = jax.random.split(jax.random.fold_in(streams_of[3], part), 4)
    queries = draw_queries(jax.random.fold_in(jax.random.fold_in(streams_of[3], part), 71), part)
    keys_values = draw_keys_values(jax.random.fold_in(jax.random.fold_in(streams_of[3], part), 71), part)
    segment_ids = jnp.searchsorted(jnp.cumsum(uneven_parts(part_keys[2], DOC_COUNT, TOKENS, DOC_MOST, 2)), jnp.arange(TOKENS), side="right").astype(jnp.int32)
    return dict(queries=queries, keys_values=keys_values, segment_ids=segment_ids)


def reference(queries, keys_values, segment_ids):
    group_size = HQ // HK
    score_scale = DH ** -0.5
    query_rows = min(512, TOKENS)
    key_span = WINDOW + query_rows
    key_table = jnp.pad(keys_values[0], ((WINDOW, 0), (0, 0)))
    value_table = jnp.pad(keys_values[1], ((WINDOW, 0), (0, 0)))
    padded_ids = jnp.pad(segment_ids, (WINDOW, 0), constant_values=-1)

    def one_block(number):
        first_row = (number * query_rows).astype(jnp.int32)
        query_block = lax.dynamic_slice_in_dim(queries, first_row, query_rows, 0)
        query_block = query_block.reshape(query_rows, HK, group_size, DH).astype(jnp.float32)
        key_block = lax.dynamic_slice_in_dim(key_table, first_row, key_span, 0).reshape(key_span, HK, DH).astype(jnp.float32)
        value_block = lax.dynamic_slice_in_dim(value_table, first_row, key_span, 0).reshape(key_span, HK, DH).astype(jnp.float32)
        query_ids = lax.dynamic_slice_in_dim(segment_ids, first_row, query_rows, 0)
        key_ids = lax.dynamic_slice_in_dim(padded_ids, first_row, key_span, 0)
        query_place = jnp.arange(query_rows, dtype=jnp.int32) + WINDOW
        key_place = jnp.arange(key_span, dtype=jnp.int32)
        distance = query_place[:, None] - key_place[None, :]
        allowed = (query_ids[:, None] == key_ids[None, :]) & (distance >= 0) & (distance < WINDOW)
        scores = jnp.einsum("qhgd,khd->hgqk", query_block, key_block) * score_scale
        scores = jnp.where(allowed, scores, -1.0e30)
        top = jnp.max(scores, axis=-1, keepdims=True)
        weights = jnp.where(allowed, jnp.exp(scores - top), 0.0)
        totals = jnp.sum(weights, axis=-1)
        rounded = lax.optimization_barrier(weights.astype(jnp.bfloat16))
        context = jnp.einsum("hgqk,khd->hgqd", rounded.astype(jnp.float32), value_block)
        result = context / totals[..., None]
        return jnp.transpose(result, (2, 0, 1, 3)).reshape(query_rows, HQ * DH).astype(jnp.bfloat16)

    blocks = lax.map(one_block, jnp.arange(TOKENS // query_rows, dtype=jnp.int32))
    return blocks.reshape(TOKENS, HQ * DH)
```

```python
import functools
import jax
import jax.numpy as jnp
from jax import lax
from jax.experimental import pallas as pl
from jax.experimental.pallas import tpu as pltpu
from jax.sharding import PartitionSpec as P

HQ = 32
HK = 8
DH = 128
WINDOW = 2048

NEG_BIG = -1e30
LOG2E = 1.4426950408889634
ID_ROWS = 16


def pack_kv(place, kv, ids, *outs, size, chunks):
    rows = kv.shape[1]
    tag = jnp.broadcast_to(ids[...].astype(jnp.float32), (ID_ROWS, rows)).astype(jnp.bfloat16)
    for c in range(chunks):
        for k in range(size):
            out = outs[c * size + k]
            start = pl.multiple_of(((place[0] ^ k) * chunks + c) * DH, DH)
            out[0:rows, :] = kv[0, :, pl.ds(start, DH)]
            out[rows : 2 * rows, :] = kv[1, :, pl.ds(start, DH)]
            out[2 * rows :, :] = tag


def pack_q(place, q, *outs, size):
    width = outs[0].shape[1]
    for k in range(size):
        start = pl.multiple_of((place[0] ^ k) * width, width)
        outs[k][...] = q[:, pl.ds(start, width)]


def unpack(place, *refs, size, chunks):
    out = refs[-1]
    width = refs[0].shape[1]
    for c in range(chunks):
        for k in range(size):
            start = pl.multiple_of(((place[0] ^ k) * chunks + c) * width, width)
            out[:, pl.ds(start, width)] = refs[c * size + k][...]


def attend(place, *refs, size, steps, first, last):
    group = HQ // HK
    q_refs, refs = refs[:size], refs[size:]
    tag_refs, refs = refs[:size], refs[size:]
    kv_refs, refs = refs[: size * len(steps)], refs[size * len(steps) :]
    if not first:
        old_stat, old_acc = refs[:2]
        refs = refs[2:]
    if last:
        outs, refs = refs[:size], refs[size:]
    else:
        new_stat, new_acc = refs[:2]
        refs = refs[2:]
    k_buf, v_buf, bias, s_buf = refs
    rows = q_refs[0].shape[0]
    keys = k_buf.shape[0]
    wide = group * rows
    tile = min(256, keys)
    member, block = place[0], place[1]
    for n in range(len(kv_refs)):
        k_buf[n * rows : (n + 1) * rows, :] = kv_refs[n][0:rows, :]
        v_buf[n * rows : (n + 1) * rows, :] = kv_refs[n][rows : 2 * rows, :]
    row_iota = lax.broadcasted_iota(jnp.int32, (rows, rows), 0)
    lane_iota = lax.broadcasted_iota(jnp.int32, (rows, rows), 1)
    scale = DH**-0.5 * LOG2E
    for i in range(size):
        q_place = (block * size + (member ^ i)) * rows + row_iota
        tag_row = tag_refs[i][0:1, :].astype(jnp.float32)
        q_tag = jnp.broadcast_to(tag_row, (rows, rows)).T
        for n in range(len(kv_refs)):
            k_place = ((block - steps[n // size]) * size + (member ^ (n % size))) * rows + lane_iota
            k_tag = jnp.broadcast_to(kv_refs[n][2 * rows : 2 * rows + 1, :].astype(jnp.float32), (rows, rows))
            distance = q_place - k_place
            allowed = (q_tag == k_tag) & (distance >= 0) & (distance < WINDOW) & (k_place >= 0)
            bias[i % 2, :, n * rows : (n + 1) * rows] = jnp.where(allowed, 0.0, NEG_BIG)
        q4 = jnp.concatenate([q_refs[i][:, h * DH : (h + 1) * DH] for h in range(group)], axis=0)
        top = None
        for t in range(0, keys, tile):
            s = lax.dot_general(
                q4, k_buf[t : t + tile, :], (((1,), (1,)), ((), ())), preferred_element_type=jnp.float32
            )
            b = bias[i % 2, :, t : t + tile]
            s = s + jnp.concatenate([b] * group, axis=0)
            s_buf[i % 2, :, t : t + tile] = s
            for u in range(0, tile, rows):
                part = s[:, u : u + rows]
                top = part if top is None else jnp.maximum(top, part)
        top = jnp.max(top, axis=1, keepdims=True)
        if not first:
            old_top = jnp.concatenate([old_stat[i, :, h : h + 1] for h in range(group)], axis=0)
            old_sum = jnp.concatenate([old_stat[i, :, group + h : group + h + 1] for h in range(group)], axis=0)
            top = jnp.maximum(top, old_top)
        total = acc = None
        for t in range(0, keys, tile):
            w = jnp.exp2((s_buf[i % 2, :, t : t + tile] - top) * scale)
            for u in range(0, tile, rows):
                part = w[:, u : u + rows]
                total = part if total is None else total + part
            add = lax.dot_general(
                w.astype(jnp.bfloat16),
                v_buf[t : t + tile, :],
                (((1,), (0,)), ((), ())),
                preferred_element_type=jnp.float32,
            )
            acc = add if acc is None else acc + add
        total = jnp.sum(total, axis=1, keepdims=True)
        if not first:
            rescale = jnp.exp2((old_top - top) * scale)
            total = total + old_sum * rescale
            acc = acc + jnp.concatenate([old_acc[i, :, h * DH : (h + 1) * DH] for h in range(group)], axis=0) * rescale
        if last:
            result = acc / total
            for h in range(group):
                outs[i][:, h * DH : (h + 1) * DH] = result[h * rows : (h + 1) * rows, :].astype(jnp.bfloat16)
        else:
            lanes = lax.broadcasted_iota(jnp.int32, (rows, DH), 1)
            stat = jnp.zeros((rows, DH), jnp.float32)
            for h in range(group):
                stat = jnp.where(lanes == h, top[h * rows : (h + 1) * rows, :], stat)
                stat = jnp.where(lanes == group + h, total[h * rows : (h + 1) * rows, :], stat)
                new_acc[i, :, h * DH : (h + 1) * DH] = acc[h * rows : (h + 1) * rows, :]
            new_stat[i, :, :] = stat


def block_size(shards):
    size = 1
    while (2 * size) ** 2 <= shards and 2 * size <= HK:
        size *= 2
    return size


def local(queries, keys_values, segment_ids, shards):
    rows = queries.shape[0]
    size = block_size(shards)
    chunks = HK // size
    width = HQ // HK * DH
    reach = min(WINDOW, rows * shards // 2)
    back = min(-(-(reach - 1) // (size * rows)), shards // size - 1)
    me = lax.axis_index("seq")
    place = jnp.stack([me % size, me // size]).astype(jnp.int32)
    smem = pl.BlockSpec(memory_space=pltpu.SMEM)
    vmem = pl.BlockSpec(memory_space=pltpu.VMEM)
    params = pltpu.CompilerParams(vmem_limit_bytes=48 * 1024 * 1024)
    bf16 = functools.partial(jax.ShapeDtypeStruct, dtype=jnp.bfloat16)
    f32 = functools.partial(jax.ShapeDtypeStruct, dtype=jnp.float32)

    def swap(x, k):
        return lax.ppermute(x, "seq", [(i, i ^ k) for i in range(shards)]) if k else x

    def onward(x):
        return lax.ppermute(x, "seq", [(i, i + size) for i in range(shards - size)])

    piece = bf16((2 * rows + ID_ROWS, DH))
    sent = pl.pallas_call(
        functools.partial(pack_kv, size=size, chunks=chunks),
        in_specs=[smem, vmem, vmem],
        out_specs=[vmem] * (chunks * size),
        out_shape=[piece] * (chunks * size),
        compiler_params=params,
        name="pack_kv",
    )(place, keys_values, segment_ids.reshape(1, rows))
    pieces = [[[swap(sent[c * size + k], k) for k in range(size)]] for c in range(chunks)]
    q_sent = pl.pallas_call(
        functools.partial(pack_q, size=size),
        in_specs=[smem, vmem],
        out_specs=[vmem] * size,
        out_shape=[bf16((rows, chunks * width))] * size,
        compiler_params=params,
        name="pack_q",
    )(place, queries)
    q_pieces = [swap(q_sent[k], k) for k in range(size)]
    for c in range(chunks):
        for d in range(back):
            pieces[c].append([onward(pieces[c][d][k]) for k in range(size)])

    def stage(c, steps, state, first, last):
        keys = len(steps) * size * rows
        args = [place] + q_pieces + pieces[0][0] + [p for d in steps for p in pieces[c][d]] + list(state)
        specs = [pl.BlockSpec((2,), lambda s: (0,), memory_space=pltpu.SMEM)]
        specs += [pl.BlockSpec((rows, width), lambda s: (0, c))] * size
        specs += [pl.BlockSpec((ID_ROWS, DH), lambda s: (2 * rows // ID_ROWS, 0))] * size
        whole = lambda a: pl.BlockSpec(a.shape, lambda s: (0,) * len(a.shape))
        specs += [whole(a) for a in args[1 + 2 * size :]]
        if last:
            shapes = [bf16((rows, width))] * size
        else:
            shapes = [f32((size, rows, DH)), f32((size, rows, width))]
        return pl.pallas_call(
            functools.partial(attend, size=size, steps=steps, first=first, last=last),
            grid=(1,),
            in_specs=specs,
            out_specs=[whole(s) for s in shapes],
            out_shape=shapes,
            scratch_shapes=[
                pltpu.VMEM((keys, DH), jnp.bfloat16),
                pltpu.VMEM((keys, DH), jnp.bfloat16),
                pltpu.VMEM((2, rows, keys), jnp.float32),
                pltpu.VMEM((2, HQ // HK * rows, keys), jnp.float32),
            ],
            compiler_params=params,
            name=f"attend_{c}_{'last' if last else 'first'}",
        )(*args)

    done = []
    for c in range(chunks):
        near = tuple(range(back)) if back else (0,)
        if back:
            state = stage(c, near, (), True, False)
            result = stage(c, (back,), state, False, True)
        else:
            result = stage(c, (0,), (), True, True)
        done += [swap(result[k], k) for k in range(size)]
    return pl.pallas_call(
        functools.partial(unpack, size=size, chunks=chunks),
        in_specs=[smem] + [vmem] * len(done),
        out_specs=vmem,
        out_shape=bf16(queries.shape),
        compiler_params=params,
        name="unpack",
    )(place, *done)


def solution(mesh):
    return jax.shard_map(
        functools.partial(local, shards=mesh.shape["seq"]),
        mesh=mesh,
        in_specs=(P(("rep", "seq"), None), P(None, ("rep", "seq"), None), P(("rep", "seq"))),
        out_specs=P(("rep", "seq"), None),
        check_vma=False,
    )
```

```python
import functools
import jax
import jax.numpy as jnp
from jax import lax
from jax.experimental import pallas as pl
from jax.experimental.pallas import tpu as pltpu
from jax.sharding import PartitionSpec as P

HQ = 32
HK = 8
DH = 128
WINDOW = 2048

GROUP = HQ // HK
NEG_BIG = -1e30
LOG2E = 1.4426950408889634
ID_ROWS = 16


def pack_kv(place, kv, ids, *outs, size, chunks):
    rows = kv.shape[1]
    tag = jnp.broadcast_to(ids[...].astype(jnp.float32), (ID_ROWS, rows)).astype(jnp.bfloat16)
    for k in range(size):
        for c in range(chunks):
            start = pl.multiple_of(((place[0] ^ k) * chunks + c) * DH, DH)
            for part in range(2):
                first = (2 * c + part) * rows
                outs[k][first : first + rows, :] = kv[part, :, pl.ds(start, DH)]
        outs[k][2 * chunks * rows :, :] = tag


def pack_q(place, q, *outs, size):
    width = outs[0].shape[1]
    for k in range(size):
        start = pl.multiple_of((place[0] ^ k) * width, width)
        outs[k][...] = q[:, pl.ds(start, width)]


def join(*refs, count, chunks, rows):
    outs = refs[count:]
    for n in range(count):
        for c in range(chunks):
            outs[c][2 * n * rows : 2 * (n + 1) * rows, :] = refs[n][2 * c * rows : 2 * (c + 1) * rows, :]
        outs[0][2 * count * rows + n * ID_ROWS : 2 * count * rows + (n + 1) * ID_ROWS, :] = refs[n][
            2 * chunks * rows :, :
        ]


def unpack(place, *refs, size, chunks):
    out = refs[-1]
    width = refs[0].shape[1]
    for c in range(chunks):
        for k in range(size):
            start = pl.multiple_of(((place[0] ^ k) * chunks + c) * width, width)
            out[:, pl.ds(start, width)] = refs[c * size + k][...]


def attend(place, *refs, chunk, size, chunks, rows, steps, first, last):
    q_refs, near, refs = refs[:size], refs[size : 2 * size], refs[2 * size :]
    far = {}
    for d in steps:
        if d:
            count = 3 if chunk else 2
            own, rest, tags = refs[0], refs[1], refs[count - 1]
            far[d] = (own, rest, tags)
            refs = refs[count:]
    if not first:
        old_top_ref, old_sum_ref, old_acc_ref = refs[:3]
        refs = refs[3:]
    if last:
        outs, refs = refs[:size], refs[size:]
    else:
        top_ref, sum_ref, acc_ref = refs[:3]
        refs = refs[3:]
    k_buf, v_buf, bias, s_buf = refs
    keys = k_buf.shape[0]
    wide = GROUP * rows
    tile = min(256, keys)
    member, block = place[0], place[1]
    tag_at = 2 * chunks * rows
    tag_rows = []
    for x, d in enumerate(steps):
        for k in range(size):
            n = x * size + k
            if d == 0 or k == 0:
                ref = near[k] if d == 0 else far[d][0]
                start, tag_ref, tag_row = 2 * chunk * rows, ref, tag_at
            else:
                ref, tag_ref = far[d][1], far[d][2]
                start, tag_row = 2 * (k - 1) * rows, 2 * (size - 1) * rows + (k - 1) * ID_ROWS
            k_buf[n * rows : (n + 1) * rows, :] = ref[start : start + rows, :]
            v_buf[n * rows : (n + 1) * rows, :] = ref[start + rows : start + 2 * rows, :]
            tag = tag_ref[tag_row : tag_row + 1, :].astype(jnp.float32)
            tag_rows.append(tag if d == 0 else jnp.where(block >= d, tag, -1.0))
    ahead = lax.broadcasted_iota(jnp.int32, (rows, rows), 0) - lax.broadcasted_iota(jnp.int32, (rows, rows), 1)
    scale = DH**-0.5 * LOG2E
    for i in range(size):
        tag_row = near[i][tag_at : tag_at + 1, :].astype(jnp.float32)
        q_tag = jnp.broadcast_to(tag_row, (rows, rows)).T
        for n, k_tag in enumerate(tag_rows):
            d = steps[n // size]
            distance = ahead + (d * size + (member ^ i) - (member ^ (n % size))) * rows
            allowed = q_tag == jnp.broadcast_to(k_tag, (rows, rows))
            if d == 0:
                allowed = allowed & (distance >= 0)
            if (d * size + size) * rows > WINDOW:
                allowed = allowed & (distance < WINDOW)
            bias[i % 2, :, n * rows : (n + 1) * rows] = jnp.where(allowed, 0.0, NEG_BIG)
        at = chunk * GROUP * DH
        q4 = jnp.concatenate([q_refs[i][:, at + h * DH : at + (h + 1) * DH] for h in range(GROUP)], axis=0)
        top = None
        for t in range(0, keys, tile):
            s = lax.dot_general(
                q4, k_buf[t : t + tile, :], (((1,), (1,)), ((), ())), preferred_element_type=jnp.float32
            )
            b = bias[i % 2, :, t : t + tile]
            s = s + jnp.concatenate([b] * GROUP, axis=0)
            s_buf[i % 2, :, t : t + tile] = s
            for u in range(0, tile, DH):
                part = s[:, u : u + DH]
                top = part if top is None else jnp.maximum(top, part)
        top = jnp.broadcast_to(jnp.max(top, axis=1, keepdims=True), (wide, DH))
        if not first:
            old_top = old_top_ref[i]
            top = jnp.maximum(top, old_top)
        total = acc = None
        for t in range(0, keys, tile):
            w = []
            for u in range(t, t + tile, DH):
                part = jnp.exp2((s_buf[i % 2, :, u : u + DH] - top) * scale)
                total = part if total is None else total + part
                w.append(part.astype(jnp.bfloat16))
            add = lax.dot_general(
                jnp.concatenate(w, axis=1),
                v_buf[t : t + tile, :],
                (((1,), (0,)), ((), ())),
                preferred_element_type=jnp.float32,
            )
            acc = add if acc is None else acc + add
        total = jnp.broadcast_to(jnp.sum(total, axis=1, keepdims=True), (wide, DH))
        if not first:
            rescale = jnp.exp2((old_top - top) * scale)
            total = total + old_sum_ref[i] * rescale
            acc = acc + old_acc_ref[i] * rescale
        if last:
            result = (acc / total).astype(jnp.bfloat16)
            for h in range(GROUP):
                outs[i][:, h * DH : (h + 1) * DH] = result[h * rows : (h + 1) * rows, :]
        else:
            top_ref[i] = top
            sum_ref[i] = total
            acc_ref[i] = acc


def layout_of(shards, rows):
    size = 1
    while (2 * size) ** 2 <= shards and 2 * size <= HK:
        size *= 2
    reach = min(WINDOW, rows * shards // 2)
    back = min(-(-(reach - 1) // (size * rows)), shards // size - 1)
    return size, HK // size, back


def local(queries, keys_values, segment_ids, shards):
    rows = queries.shape[0]
    size, chunks, back = layout_of(shards, rows)
    width = GROUP * DH
    me = lax.axis_index("seq")
    place = jnp.stack([me & (size - 1), me >> (size.bit_length() - 1)]).astype(jnp.int32)
    smem = pl.BlockSpec(memory_space=pltpu.SMEM)
    vmem = pl.BlockSpec(memory_space=pltpu.VMEM)
    params = pltpu.CompilerParams(vmem_limit_bytes=48 * 1024 * 1024)
    bf16 = functools.partial(jax.ShapeDtypeStruct, dtype=jnp.bfloat16)
    f32 = functools.partial(jax.ShapeDtypeStruct, dtype=jnp.float32)

    def call(body, shapes, args, scratch=()):
        return pl.pallas_call(
            body,
            in_specs=[smem if a is place else vmem for a in args],
            out_specs=[vmem] * len(shapes),
            out_shape=shapes,
            scratch_shapes=scratch,
            compiler_params=params,
        )(*args)

    def swap(x, k):
        return lax.ppermute(x, "seq", [(i, i ^ k) for i in range(shards)]) if k else x

    def onward(x):
        return lax.ppermute(x, "seq", [(i, i + size) for i in range(shards - size)])

    sent = call(
        functools.partial(pack_kv, size=size, chunks=chunks),
        [bf16((2 * chunks * rows + ID_ROWS, DH))] * size,
        [place, keys_values, segment_ids.reshape(1, rows)],
    )
    near = [swap(sent[k], k) for k in range(size)]
    q_sent = call(functools.partial(pack_q, size=size), [bf16((rows, chunks * width))] * size, [place, queries])
    q_parts = [swap(q_sent[k], k) for k in range(size)]
    count = size - 1
    rest_shapes = [bf16((count * (2 * rows + (0 if c else ID_ROWS)), DH)) for c in range(chunks)]
    far_own, far_rest = [sent[0]], []
    if back:
        far_rest.append(call(functools.partial(join, count=count, chunks=chunks, rows=rows), rest_shapes, near[1:]))
    for d in range(1, back + 1):
        far_own.append(onward(far_own[d - 1]))
        far_rest.append([onward(far_rest[d - 1][c]) for c in range(chunks)])

    def stage(c, steps, state, first, last):
        keys = len(steps) * size * rows
        args = [place] + q_parts + near
        for d in steps:
            if d:
                args += [far_own[d], far_rest[d][c]] + ([far_rest[d][0]] if c else [])
        args += list(state)
        shapes = [bf16((rows, width))] * size if last else [f32((size, GROUP * rows, DH))] * 3
        scratch = [
            pltpu.VMEM((keys, DH), jnp.bfloat16),
            pltpu.VMEM((keys, DH), jnp.bfloat16),
            pltpu.VMEM((2, rows, keys), jnp.float32),
            pltpu.VMEM((2, GROUP * rows, keys), jnp.float32),
        ]
        body = functools.partial(
            attend, chunk=c, size=size, chunks=chunks, rows=rows, steps=steps, first=first, last=last
        )
        return call(body, shapes, args, scratch)

    states = [()] * chunks
    if back:
        states = [stage(c, tuple(range(back)), (), True, False) for c in range(chunks)]
    done = []
    for c in range(chunks):
        result = stage(c, (back,), states[c], not back, True)
        done += [swap(result[k], k) for k in range(size)]
    return call(functools.partial(unpack, size=size, chunks=chunks), [bf16(queries.shape)], [place] + done)[0]


def solution(mesh):
    shards = mesh.shape["seq"]

    def body(queries, keys_values, segment_ids):
        return local(queries, keys_values, segment_ids, shards)

    return jax.shard_map(
        body,
        mesh=mesh,
        in_specs=(P(("rep", "seq"), None), P(None, ("rep", "seq"), None), P(("rep", "seq"))),
        out_specs=P(("rep", "seq"), None),
        check_vma=False,
    )
```

```python
import functools
import jax
import jax.numpy as jnp
from jax import lax
from jax.experimental import pallas as pl
from jax.experimental.pallas import tpu as pltpu
from jax.sharding import PartitionSpec as P

HQ = 32
HK = 8
DH = 128
WINDOW = 2048

GROUP = HQ // HK
NEG_BIG = -1e30
LOG2E = 1.4426950408889634
ID_ROWS = 16
IDS = 32


def pack(place, kv, ids, q, *refs, size, chunks):
    kv_outs, q_outs, (ids_buf, sems) = refs[:size], refs[size : 2 * size], refs[2 * size :]
    rows = kv.shape[1]
    width = q_outs[0].shape[1]
    moves = [(ids, ids_buf)]
    for k in range(size):
        for c in range(chunks):
            start = pl.multiple_of(((place[0] ^ k) * chunks + c) * DH, DH)
            for part in range(2):
                first = (2 * c + part) * rows
                moves.append((kv.at[part, :, pl.ds(start, DH)], kv_outs[k].at[pl.ds(first, rows), :]))
    for k in range(size):
        moves.append((q.at[:, pl.ds(pl.multiple_of((place[0] ^ k) * width, width), width)], q_outs[k]))
    copies = [pltpu.make_async_copy(a, b, sems.at[n]) for n, (a, b) in enumerate(moves)]
    for copy in copies:
        copy.start()
    copies[0].wait()
    tag = jnp.broadcast_to(ids_buf[...].astype(jnp.float32), (ID_ROWS, rows)).astype(jnp.bfloat16)
    for k in range(size):
        kv_outs[k][2 * chunks * rows :, :] = tag
    for copy in copies[1:]:
        copy.wait()


def join(*refs, count, chunks, rows):
    outs = refs[count:]
    for n in range(count):
        for c in range(chunks):
            outs[c][2 * n * rows : 2 * (n + 1) * rows, :] = refs[n][2 * c * rows : 2 * (c + 1) * rows, :]
        outs[0][2 * count * rows + n * ID_ROWS : 2 * count * rows + (n + 1) * ID_ROWS, :] = refs[n][
            2 * chunks * rows :, :
        ]


def unpack(place, *refs, size, chunks):
    out, sems = refs[-2:]
    width = refs[0].shape[1]
    copies = []
    for c in range(chunks):
        for k in range(size):
            start = pl.multiple_of(((place[0] ^ k) * chunks + c) * width, width)
            n = c * size + k
            copies.append(pltpu.make_async_copy(refs[n], out.at[:, pl.ds(start, width)], sems.at[n]))
    for copy in copies:
        copy.start()
    for copy in copies:
        copy.wait()


def attend(place, *refs, chunk, size, chunks, rows, steps, first, last):
    q_refs, near, refs = refs[:size], refs[size : 2 * size], refs[2 * size :]
    far = {}
    for d in steps:
        if d:
            count = 3 if chunk else 2
            far[d] = (refs[0], refs[1], refs[count - 1])
            refs = refs[count:]
    if not first:
        old_top_ref, old_sum_ref, old_acc_ref = refs[:3]
        refs = refs[3:]
    if last:
        outs, refs = refs[:size], refs[size:]
    else:
        top_ref, sum_ref, acc_ref = refs[:3]
        refs = refs[3:]
    q_buf, k_buf, v_buf, s_buf, w_buf = refs
    keys = k_buf.shape[0]
    tile = min(256, keys)
    member, block = place[0], place[1]
    tag_at = 2 * chunks * rows
    lane = lax.broadcasted_iota(jnp.int32, (rows, DH), 1)
    lane_tag = lane.astype(jnp.float32)
    after = lane > lax.broadcasted_iota(jnp.int32, (rows, DH), 0)
    scale = DH**-0.5 * LOG2E

    def column(tag_row):
        return jnp.broadcast_to(tag_row.astype(jnp.float32), (rows, DH)).T

    for x, d in enumerate(steps):
        for k in range(size):
            n = x * size + k
            if d == 0 or k == 0:
                ref = near[k] if d == 0 else far[d][0]
                start, tag_ref, tag_row = 2 * chunk * rows, ref, tag_at
            else:
                ref, tag_ref = far[d][1], far[d][2]
                start, tag_row = 2 * (k - 1) * rows, 2 * (size - 1) * rows + (k - 1) * ID_ROWS
            at = slice(n * rows, (n + 1) * rows)
            k_buf[at, :DH] = ref[start : start + rows, :]
            v_buf[at, :] = ref[start + rows : start + 2 * rows, :]
            other = column(tag_ref[tag_row : tag_row + 1, :]) != lane_tag
            if d:
                blocked = (other & (lane < IDS)) | (block < d)
            else:
                blocked = (other & (lane < IDS)) | (lane == IDS + (member ^ k))
            k_buf[at, DH:] = jnp.where(blocked, NEG_BIG, 0.0).astype(jnp.bfloat16)

    def scores(i):
        own = column(near[i][tag_at : tag_at + 1, :]) == lane_tag
        later = (lane > IDS + (member ^ i)) & (lane < IDS + size)
        mark = jnp.where(own | later, 1.0, 0.0).astype(jnp.bfloat16)
        at = chunk * GROUP * DH
        for h in range(GROUP):
            q_buf[i % 2, h * rows : (h + 1) * rows, :DH] = q_refs[i][:, at + h * DH : at + (h + 1) * DH]
            q_buf[i % 2, h * rows : (h + 1) * rows, DH:] = mark
        for t in range(0, keys, tile):
            s_buf[i % 2, :, t : t + tile] = lax.dot_general(
                q_buf[i % 2],
                k_buf[t : t + tile, :],
                (((1,), (1,)), ((), ())),
                preferred_element_type=jnp.float32,
            )

    def softmax(i):
        kept = []
        for h in range(GROUP):
            at = slice(h * rows, (h + 1) * rows)
            top = None
            for t in range(0, keys, DH):
                part = s_buf[i % 2, at, t : t + DH]
                if steps[0] == 0 and t == i * rows and rows == DH:
                    part = jnp.where(after, NEG_BIG, part)
                    s_buf[i % 2, at, t : t + DH] = part
                top = part if top is None else jnp.maximum(top, part)
            top = jnp.broadcast_to(jnp.max(top, axis=1, keepdims=True), (rows, DH))
            if not first:
                top = jnp.maximum(top, old_top_ref[i, at, :])
            total = None
            for t in range(0, keys, DH):
                part = jnp.exp2((s_buf[i % 2, at, t : t + DH] - top) * scale)
                total = part if total is None else total + part
                w_buf[i % 2, at, t : t + DH] = part.astype(jnp.bfloat16)
            total = jnp.broadcast_to(jnp.sum(total, axis=1, keepdims=True), (rows, DH))
            if not first:
                rescale = jnp.exp2((old_top_ref[i, at, :] - top) * scale)
                total = total + old_sum_ref[i, at, :] * rescale
            else:
                rescale = None
            if not last:
                top_ref[i, at, :] = top
                sum_ref[i, at, :] = total
            kept.append((total, rescale))
        return kept

    def context(i, kept):
        acc = jnp.dot(w_buf[i % 2], v_buf[...], preferred_element_type=jnp.float32)
        for h, (total, rescale) in enumerate(kept):
            at = slice(h * rows, (h + 1) * rows)
            part = acc[at, :]
            if rescale is not None:
                part = part + old_acc_ref[i, at, :] * rescale
            if last:
                outs[i][:, h * DH : (h + 1) * DH] = (part / total).astype(jnp.bfloat16)
            else:
                acc_ref[i, at, :] = part

    scores(0)
    for i in range(size):
        if i + 1 < size:
            scores(i + 1)
        context(i, softmax(i))


def layout_of(shards, rows):
    size = 1
    while (2 * size) ** 2 <= shards and 2 * size <= HK:
        size *= 2
    reach = min(WINDOW, rows * shards // 2)
    back = min(-(-(reach - 1) // (size * rows)), shards // size - 1)
    return size, HK // size, back


def local(queries, keys_values, segment_ids, shards):
    rows = queries.shape[0]
    size, chunks, back = layout_of(shards, rows)
    width = GROUP * DH
    me = lax.axis_index("seq")
    place = jnp.stack([me & (size - 1), me >> (size.bit_length() - 1)]).astype(jnp.int32)
    smem = pl.BlockSpec(memory_space=pltpu.SMEM)
    vmem = pl.BlockSpec(memory_space=pltpu.VMEM)
    hbm = pl.BlockSpec(memory_space=pltpu.HBM)
    params = pltpu.CompilerParams(vmem_limit_bytes=48 * 1024 * 1024)
    bf16 = functools.partial(jax.ShapeDtypeStruct, dtype=jnp.bfloat16)
    f32 = functools.partial(jax.ShapeDtypeStruct, dtype=jnp.float32)

    def call(body, shapes, args, scratch=(), far_in=(), far_out=False):
        return pl.pallas_call(
            body,
            in_specs=[smem if a is place else hbm if n in far_in else vmem for n, a in enumerate(args)],
            out_specs=[hbm if far_out else vmem] * len(shapes),
            out_shape=shapes,
            scratch_shapes=scratch,
            compiler_params=params,
        )(*args)

    def swap(x, k):
        return lax.ppermute(x, "seq", [(i, i ^ k) for i in range(shards)]) if k else x

    def onward(x):
        return lax.ppermute(x, "seq", [(i, i + size) for i in range(shards - size)])

    packed = call(
        functools.partial(pack, size=size, chunks=chunks),
        [bf16((2 * chunks * rows + ID_ROWS, DH))] * size + [bf16((rows, chunks * width))] * size,
        [place, keys_values, segment_ids.reshape(1, rows), queries],
        [pltpu.VMEM((1, rows), jnp.int32), pltpu.SemaphoreType.DMA((1 + 2 * HK + size,))],
        far_in=(1, 2, 3),
    )
    sent, q_sent = packed[:size], packed[size:]
    near = [swap(sent[k], k) for k in range(size)]
    q_parts = [swap(q_sent[k], k) for k in range(size)]
    count = size - 1
    rest_shapes = [bf16((count * (2 * rows + (0 if c else ID_ROWS)), DH)) for c in range(chunks)]
    far_own, far_rest = [sent[0]], []
    if back:
        far_rest.append(call(functools.partial(join, count=count, chunks=chunks, rows=rows), rest_shapes, near[1:]))
    for d in range(1, back + 1):
        far_own.append(onward(far_own[d - 1]))
        far_rest.append([onward(far_rest[d - 1][c]) for c in range(chunks)])

    def stage(c, steps, state, first, last):
        keys = len(steps) * size * rows
        args = [place] + q_parts + near
        for d in steps:
            if d:
                args += [far_own[d], far_rest[d][c]] + ([far_rest[d][0]] if c else [])
        args += list(state)
        shapes = [bf16((rows, width))] * size if last else [f32((size, GROUP * rows, DH))] * 3
        scratch = [
            pltpu.VMEM((2, GROUP * rows, 2 * DH), jnp.bfloat16),
            pltpu.VMEM((keys, 2 * DH), jnp.bfloat16),
            pltpu.VMEM((keys, DH), jnp.bfloat16),
            pltpu.VMEM((2, GROUP * rows, keys), jnp.float32),
            pltpu.VMEM((2, GROUP * rows, keys), jnp.bfloat16),
        ]
        body = functools.partial(
            attend, chunk=c, size=size, chunks=chunks, rows=rows, steps=steps, first=first, last=last
        )
        return call(body, shapes, args, scratch)

    states = [()] * chunks
    if back:
        states = [stage(c, tuple(range(back)), (), True, False) for c in range(chunks)]
    done = []
    for c in range(chunks):
        result = stage(c, (back,), states[c], not back, True)
        done += [swap(result[k], k) for k in range(size)]
    return call(
        functools.partial(unpack, size=size, chunks=chunks),
        [bf16(queries.shape)],
        [place] + done,
        [pltpu.SemaphoreType.DMA((len(done),))],
        far_out=True,
    )[0]


def solution(mesh):
    shards = mesh.shape["seq"]

    def body(queries, keys_values, segment_ids):
        return local(queries, keys_values, segment_ids, shards)

    return jax.shard_map(
        body,
        mesh=mesh,
        in_specs=(P(("rep", "seq"), None), P(None, ("rep", "seq"), None), P(("rep", "seq"))),
        out_specs=P(("rep", "seq"), None),
        check_vma=False,
    )
```

```python
import functools
import jax
import jax.numpy as jnp
from jax import lax
from jax.experimental import pallas as pl
from jax.experimental.pallas import tpu as pltpu
from jax.sharding import PartitionSpec as P

HQ = 32
HK = 8
DH = 128
WINDOW = 2048

GROUP = HQ // HK
NEG_BIG = -1e30
LOG2E = 1.4426950408889634
ID_ROWS = 16


def pack(place, kv, ids, q, *refs, size, chunks):
    kv_outs, q_outs, (ids_buf, sems) = refs[:size], refs[size : 2 * size], refs[2 * size :]
    rows = kv.shape[1]
    width = q_outs[0].shape[1]
    moves = [(ids, ids_buf)]
    for k in range(size):
        for c in range(chunks):
            start = pl.multiple_of(((place[0] ^ k) * chunks + c) * DH, DH)
            for part in range(2):
                first = (2 * c + part) * rows
                moves.append((kv.at[part, :, pl.ds(start, DH)], kv_outs[k].at[pl.ds(first, rows), :]))
    for k in range(size):
        moves.append((q.at[:, pl.ds(pl.multiple_of((place[0] ^ k) * width, width), width)], q_outs[k]))
    copies = [pltpu.make_async_copy(a, b, sems.at[n]) for n, (a, b) in enumerate(moves)]
    for copy in copies:
        copy.start()
    copies[0].wait()
    tag = jnp.broadcast_to(ids_buf[...].astype(jnp.float32), (ID_ROWS, rows)).astype(jnp.bfloat16)
    for k in range(size):
        kv_outs[k][2 * chunks * rows :, :] = tag
    for copy in copies[1:]:
        copy.wait()


def join(*refs, count, chunks, rows):
    outs = refs[count:]
    for n in range(count):
        for c in range(chunks):
            outs[c][2 * n * rows : 2 * (n + 1) * rows, :] = refs[n][2 * c * rows : 2 * (c + 1) * rows, :]
        outs[0][2 * count * rows + n * ID_ROWS : 2 * count * rows + (n + 1) * ID_ROWS, :] = refs[n][
            2 * chunks * rows :, :
        ]


def unpack(place, *refs, size, chunks):
    out, sems = refs[-2:]
    width = refs[0].shape[1]
    copies = []
    for c in range(chunks):
        for k in range(size):
            start = pl.multiple_of(((place[0] ^ k) * chunks + c) * width, width)
            n = c * size + k
            copies.append(pltpu.make_async_copy(refs[n], out.at[:, pl.ds(start, width)], sems.at[n]))
    for copy in copies:
        copy.start()
    for copy in copies:
        copy.wait()


def attend(place, *refs, chunk, size, chunks, rows, reach, steps, first, last):
    q_refs, near, refs = refs[:size], refs[size : 2 * size], refs[2 * size :]
    far = {}
    for d in steps:
        if d:
            count = 3 if chunk else 2
            far[d] = (refs[0], refs[1], refs[count - 1])
            refs = refs[count:]
    if not first:
        old_top_ref, old_sum_ref, old_acc_ref = refs[:3]
        refs = refs[3:]
    if last:
        outs, refs = refs[:size], refs[size:]
    else:
        top_ref, sum_ref, acc_ref = refs[:3]
        refs = refs[3:]
    q_buf, k_buf, v_buf, tag_buf, bias, s_buf, o_buf = refs
    wide = GROUP * rows
    member, block = place[0], place[1]
    tag_at = 2 * chunks * rows
    blocks = sorted(set(steps) | {0}, reverse=True)
    for k in range(size):
        spot = member ^ k
        for d in blocks:
            if d == 0 or k == 0:
                ref = near[k] if d == 0 else far[d][0]
                start, tag_ref, tag_row = 2 * chunk * rows, ref, tag_at
            else:
                ref, tag_ref = far[d][1], far[d][2]
                start, tag_row = 2 * (k - 1) * rows, 2 * (size - 1) * rows + (k - 1) * ID_ROWS
            at = pl.ds(pl.multiple_of((blocks.index(d) * size + spot) * rows, rows), rows)
            if d in steps:
                k_buf[at, :] = ref[start : start + rows, :]
                v_buf[at, :] = ref[start + rows : start + 2 * rows, :]
            tag = tag_ref[tag_row : tag_row + 1, :].astype(jnp.float32)
            if d:
                tag = jnp.where(block >= d, tag, -1.0)
            at = pl.ds(pl.multiple_of((blocks.index(d) * size + spot) * 8, 8), 8)
            tag_buf[at, :] = jnp.broadcast_to(tag, (8, rows))
        for h in range(GROUP):
            at = pl.ds(pl.multiple_of(spot * wide + h * rows, rows), rows)
            col = (chunk * GROUP + h) * DH
            q_buf[at, :] = q_refs[k][:, col : col + DH]
    ahead = lax.broadcasted_iota(jnp.int32, (rows, rows), 0) - lax.broadcasted_iota(jnp.int32, (rows, rows), 1)
    scale = DH**-0.5 * LOG2E
    for j in range(size):
        seen = []
        for d in steps:
            for n in range(size):
                apart = d * size + j - n
                if apart >= 0 and apart * rows - (rows - 1) < reach:
                    seen.append((blocks.index(d) * size + n, apart))
        seen.sort()
        low, high = seen[0][0] * rows, (seen[-1][0] + 1) * rows
        turn = j % 2
        spot = blocks.index(0) * size + j
        q_tag = jnp.broadcast_to(tag_buf[spot * 8 : spot * 8 + 1, :], (rows, rows)).T
        for spot, apart in seen:
            allowed = q_tag == jnp.broadcast_to(tag_buf[spot * 8 : spot * 8 + 1, :], (rows, rows))
            if apart == 0:
                allowed = allowed & (ahead >= 0)
            if apart * rows + rows > WINDOW:
                allowed = allowed & (ahead + apart * rows < WINDOW)
            bias[turn, :, spot * rows : (spot + 1) * rows] = jnp.where(allowed, 0.0, NEG_BIG)
        q4 = q_buf[j * wide : (j + 1) * wide, :]
        tiles = [(t, min(256, high - t)) for t in range(low, high, 256)]
        top = None
        for t, w in tiles:
            s = lax.dot_general(
                q4, k_buf[t : t + w, :], (((1,), (1,)), ((), ())), preferred_element_type=jnp.float32
            )
            s = s + jnp.concatenate([bias[turn, :, t : t + w]] * GROUP, axis=0)
            s_buf[turn, :, t : t + w] = s
            for u in range(0, w, DH):
                part = s[:, u : u + DH]
                top = part if top is None else jnp.maximum(top, part)
        top = jnp.broadcast_to(jnp.max(top, axis=1, keepdims=True), (wide, DH))
        if not first:
            old_top = old_top_ref[j]
            top = jnp.maximum(top, old_top)
        total = acc = None
        for t, w in tiles:
            parts = []
            for u in range(t, t + w, DH):
                part = jnp.exp2((s_buf[turn, :, u : u + DH] - top) * scale)
                total = part if total is None else total + part
                parts.append(part.astype(jnp.bfloat16))
            add = jnp.dot(jnp.concatenate(parts, axis=1), v_buf[t : t + w, :], preferred_element_type=jnp.float32)
            acc = add if acc is None else acc + add
        total = jnp.broadcast_to(jnp.sum(total, axis=1, keepdims=True), (wide, DH))
        if not first:
            rescale = jnp.exp2((old_top - top) * scale)
            total = total + old_sum_ref[j] * rescale
            acc = acc + old_acc_ref[j] * rescale
        if last:
            result = (acc / total).astype(jnp.bfloat16)
            for h in range(GROUP):
                o_buf[j * rows : (j + 1) * rows, h * DH : (h + 1) * DH] = result[h * rows : (h + 1) * rows, :]
        else:
            top_ref[j] = top
            sum_ref[j] = total
            acc_ref[j] = acc
    if last:
        for k in range(size):
            outs[k][...] = o_buf[pl.ds(pl.multiple_of((member ^ k) * rows, rows), rows), :]


def scratch_of(size, rows, steps):
    spots = len(set(steps) | {0}) * size
    keys = spots * rows
    return [
        pltpu.VMEM((size * GROUP * rows, DH), jnp.bfloat16),
        pltpu.VMEM((keys, DH), jnp.bfloat16),
        pltpu.VMEM((keys, DH), jnp.bfloat16),
        pltpu.VMEM((spots * 8, rows), jnp.float32),
        pltpu.VMEM((2, rows, keys), jnp.float32),
        pltpu.VMEM((2, GROUP * rows, keys), jnp.float32),
        pltpu.VMEM((size * rows, GROUP * DH), jnp.bfloat16),
    ]


def layout_of(shards, rows):
    size = 1
    while (2 * size) ** 2 <= shards and 2 * size <= HK:
        size *= 2
    reach = min(WINDOW, rows * shards // 2)
    back = min(-(-(reach - 1) // (size * rows)), shards // size - 1)
    return size, HK // size, back, reach


def local(queries, keys_values, segment_ids, shards):
    rows = queries.shape[0]
    size, chunks, back, reach = layout_of(shards, rows)
    width = GROUP * DH
    me = lax.axis_index("seq")
    place = jnp.stack([me & (size - 1), me >> (size.bit_length() - 1)]).astype(jnp.int32)
    smem = pl.BlockSpec(memory_space=pltpu.SMEM)
    vmem = pl.BlockSpec(memory_space=pltpu.VMEM)
    hbm = pl.BlockSpec(memory_space=pltpu.HBM)
    params = pltpu.CompilerParams(vmem_limit_bytes=48 * 1024 * 1024)
    bf16 = functools.partial(jax.ShapeDtypeStruct, dtype=jnp.bfloat16)
    f32 = functools.partial(jax.ShapeDtypeStruct, dtype=jnp.float32)

    def call(body, shapes, args, scratch=(), far_in=(), far_out=False):
        return pl.pallas_call(
            body,
            in_specs=[smem if a is place else hbm if n in far_in else vmem for n, a in enumerate(args)],
            out_specs=[hbm if far_out else vmem] * len(shapes),
            out_shape=shapes,
            scratch_shapes=scratch,
            compiler_params=params,
        )(*[pltpu.with_memory_space_constraint(a, pltpu.HBM) if n in far_in else a for n, a in enumerate(args)])

    def swap(x, k):
        return lax.ppermute(x, "seq", [(i, i ^ k) for i in range(shards)]) if k else x

    def onward(x, d):
        return lax.ppermute(x, "seq", [(i, i + size) for i in range((d - 1) * size, shards - size)])

    packed = call(
        functools.partial(pack, size=size, chunks=chunks),
        [bf16((2 * chunks * rows + ID_ROWS, DH))] * size + [bf16((rows, chunks * width))] * size,
        [place, keys_values, segment_ids.reshape(1, rows), queries],
        [pltpu.VMEM((1, rows), jnp.int32), pltpu.SemaphoreType.DMA((1 + 2 * HK + size,))],
        far_in=(1, 2, 3),
    )
    sent, q_sent = packed[:size], packed[size:]
    near = [swap(sent[k], k) for k in range(size)]
    q_parts = [swap(q_sent[k], k) for k in range(size)]
    count = size - 1
    rest_shapes = [bf16((count * (2 * rows + (0 if c else ID_ROWS)), DH)) for c in range(chunks)]
    far_own, far_rest = [sent[0]], []
    if back:
        far_rest.append(call(functools.partial(join, count=count, chunks=chunks, rows=rows), rest_shapes, near[1:]))
    for d in range(1, back + 1):
        far_own.append(onward(far_own[d - 1], d))
        far_rest.append([onward(far_rest[d - 1][c], d) for c in range(chunks)])

    def stage(c, steps, state, first, last):
        args = [place] + q_parts + near
        for d in steps:
            if d:
                args += [far_own[d], far_rest[d][c]] + ([far_rest[d][0]] if c else [])
        args += list(state)
        shapes = [bf16((rows, width))] * size if last else [f32((size, GROUP * rows, DH))] * 3
        scratch = scratch_of(size, rows, steps)
        body = functools.partial(
            attend, chunk=c, size=size, chunks=chunks, rows=rows, reach=reach, steps=steps, first=first, last=last
        )
        return call(body, shapes, args, scratch)

    states = [()] * chunks
    if back:
        states = [stage(c, tuple(range(back)), (), True, False) for c in range(chunks)]
    done = []
    for c in range(chunks):
        result = stage(c, (back,), states[c], not back, True)
        done += [swap(result[k], k) for k in range(size)]
    return call(
        functools.partial(unpack, size=size, chunks=chunks),
        [bf16(queries.shape)],
        [place] + done,
        [pltpu.SemaphoreType.DMA((len(done),))],
        far_out=True,
    )[0]


def solution(mesh):
    shards = mesh.shape["seq"]

    def body(queries, keys_values, segment_ids):
        return local(queries, keys_values, segment_ids, shards)

    return jax.shard_map(
        body,
        mesh=mesh,
        in_specs=(P(("rep", "seq"), None), P(None, ("rep", "seq"), None), P(("rep", "seq"))),
        out_specs=P(("rep", "seq"), None),
        check_vma=False,
    )
```

```python
import functools
import jax
import jax.numpy as jnp
from jax import lax
from jax.experimental import pallas as pl
from jax.experimental.pallas import tpu as pltpu
from jax.sharding import PartitionSpec as P

HQ = 32
HK = 8
DH = 128
WINDOW = 2048

GROUP = HQ // HK
NEG_BIG = -1e30
LOG2E = 1.4426950408889634
ID_ROWS = 16


def pack(place, kv, ids, q, *refs, size, chunks):
    kv_outs, q_outs, (ids_buf, sems) = refs[:size], refs[size : 2 * size], refs[2 * size :]
    rows = kv.shape[1]
    width = q_outs[0].shape[1]
    moves = [(ids, ids_buf)]
    for k in range(size):
        for c in range(chunks):
            start = pl.multiple_of(((place[0] ^ k) * chunks + c) * DH, DH)
            for part in range(2):
                first = (2 * c + part) * rows
                moves.append((kv.at[part, :, pl.ds(start, DH)], kv_outs[k].at[pl.ds(first, rows), :]))
    for k in range(size):
        moves.append((q.at[:, pl.ds(pl.multiple_of((place[0] ^ k) * width, width), width)], q_outs[k]))
    copies = [pltpu.make_async_copy(a, b, sems.at[n]) for n, (a, b) in enumerate(moves)]
    for copy in copies:
        copy.start()
    copies[0].wait()
    tag = jnp.broadcast_to(ids_buf[...].astype(jnp.float32), (ID_ROWS, rows)).astype(jnp.bfloat16)
    for k in range(size):
        kv_outs[k][2 * chunks * rows :, :] = tag
    for copy in copies[1:]:
        copy.wait()


def join(*refs, count, chunks, rows):
    outs = refs[count:]
    for n in range(count):
        for c in range(chunks):
            outs[c][2 * n * rows : 2 * (n + 1) * rows, :] = refs[n][2 * c * rows : 2 * (c + 1) * rows, :]
        outs[0][2 * count * rows + n * ID_ROWS : 2 * count * rows + (n + 1) * ID_ROWS, :] = refs[n][
            2 * chunks * rows :, :
        ]


def unpack(place, *refs, size, chunks):
    out, sems = refs[-2:]
    width = refs[0].shape[1]
    copies = []
    for c in range(chunks):
        for k in range(size):
            start = pl.multiple_of(((place[0] ^ k) * chunks + c) * width, width)
            n = c * size + k
            copies.append(pltpu.make_async_copy(refs[n], out.at[:, pl.ds(start, width)], sems.at[n]))
    for copy in copies:
        copy.start()
    for copy in copies:
        copy.wait()


def attend(place, *refs, chunk, size, chunks, rows, reach, steps, first, last):
    q_refs, near, refs = refs[:size], refs[size : 2 * size], refs[2 * size :]
    far = {}
    for d in steps:
        if d:
            count = 3 if chunk else 2
            far[d] = (refs[0], refs[1], refs[count - 1])
            refs = refs[count:]
    if not first:
        old_top_ref, old_sum_ref, old_acc_ref = refs[:3]
        refs = refs[3:]
    if last:
        outs, refs = refs[:size], refs[size:]
    else:
        top_ref, sum_ref, acc_ref = refs[:3]
        refs = refs[3:]
    q_buf, k_buf, v_buf, tag_buf, col_buf, s_buf, w_buf, o_buf, stat_buf = refs
    wide = GROUP * rows
    member, block = place[0], place[1]
    tag_at = 2 * chunks * rows
    blocks = sorted(set(steps) | {0}, reverse=True)
    for k in range(size):
        spot = member ^ k
        for d in blocks:
            if d == 0 or k == 0:
                ref = near[k] if d == 0 else far[d][0]
                start, tag_ref, tag_row = 2 * chunk * rows, ref, tag_at
            else:
                ref, tag_ref = far[d][1], far[d][2]
                start, tag_row = 2 * (k - 1) * rows, 2 * (size - 1) * rows + (k - 1) * ID_ROWS
            place_in = blocks.index(d) * size + spot
            tag = tag_ref[tag_row : tag_row + 1, :].astype(jnp.float32)
            if d:
                tag = jnp.where(block >= d, tag, -1.0)
            if d in steps:
                at = pl.ds(pl.multiple_of(place_in * rows, rows), rows)
                k_buf[at, :] = ref[start : start + rows, :]
                v_buf[:, at] = ref[start + rows : start + 2 * rows, :].T
                col_buf[at, :] = jnp.broadcast_to(tag, (rows, rows)).T
            if d == 0:
                tag_buf[pl.ds(pl.multiple_of(spot * 8, 8), 8), :] = jnp.broadcast_to(tag, (8, rows))
        for h in range(GROUP):
            at = pl.ds(pl.multiple_of(spot * wide + h * rows, rows), rows)
            col = (chunk * GROUP + h) * DH
            q_buf[at, :] = q_refs[k][:, col : col + DH]
    ahead = lax.broadcasted_iota(jnp.int32, (rows, rows), 1) - lax.broadcasted_iota(jnp.int32, (rows, rows), 0)
    scale = DH**-0.5 * LOG2E

    def reached(j):
        seen = {}
        for d in steps:
            for n in range(size):
                apart = d * size + j - n
                if apart >= 0 and apart * rows - (rows - 1) < reach:
                    seen[blocks.index(d) * size + n] = apart
        return min(seen) * rows, (max(seen) + 1) * rows, seen

    def scores(j):
        low, high, seen = reached(j)
        q_tag = tag_buf[j * 8 : j * 8 + 1, :]
        s = lax.dot_general(
            k_buf[low:high, :],
            q_buf[j * wide : (j + 1) * wide, :],
            (((1,), (1,)), ((), ())),
            preferred_element_type=jnp.float32,
        )
        top = None
        for u in range(low, high, rows):
            apart = seen[u // rows]
            allowed = col_buf[u : u + rows, :] == q_tag
            if apart == 0:
                allowed = allowed & (ahead >= 0)
            if apart * rows + rows > WINDOW:
                allowed = allowed & (ahead + apart * rows < WINDOW)
            bias = jnp.where(allowed, 0.0, NEG_BIG)
            part = s[u - low : u - low + rows, :] + jnp.concatenate([bias] * GROUP, axis=1)
            s_buf[j % 2, u : u + rows, :] = part
            part = jnp.max(part.reshape(rows // 8, 8, wide), axis=0)
            top = part if top is None else jnp.maximum(top, part)
        stat_buf[j % 2] = top

    def softmax(j):
        low, high, _ = reached(j)
        top = jnp.max(stat_buf[j % 2], axis=0, keepdims=True)
        if not first:
            top = jnp.maximum(top, old_top_ref[j * 8 : j * 8 + 1, :])
        total = None
        for u in range(low, high, rows):
            part = jnp.exp2((s_buf[j % 2, u : u + rows, :] - top) * scale)
            w_buf[j % 2, u : u + rows, :] = part.astype(jnp.bfloat16)
            part = jnp.sum(part.reshape(rows // 8, 8, wide), axis=0)
            total = part if total is None else total + part
        total = jnp.sum(total, axis=0, keepdims=True)
        if not first:
            rescale = jnp.exp2((old_top_ref[j * 8 : j * 8 + 1, :] - top) * scale)
            total = total + old_sum_ref[j * 8 : j * 8 + 1, :] * rescale
            stat_buf[2 + j % 2] = jnp.broadcast_to(rescale, (8, wide))
        if last:
            stat_buf[4 + j % 2] = jnp.broadcast_to(1.0 / total, (8, wide))
        else:
            top_ref[j * 8 : (j + 1) * 8, :] = jnp.broadcast_to(top, (8, wide))
            sum_ref[j * 8 : (j + 1) * 8, :] = jnp.broadcast_to(total, (8, wide))

    def context(j):
        low, high, _ = reached(j)
        acc = jnp.dot(v_buf[:, low:high], w_buf[j % 2, low:high, :], preferred_element_type=jnp.float32)
        if not first:
            acc = acc + old_acc_ref[j] * stat_buf[2 + j % 2, 0:1, :]
        if last:
            acc = acc * stat_buf[4 + j % 2, 0:1, :]
            for h in range(GROUP):
                o_buf[j * rows : (j + 1) * rows, h * DH : (h + 1) * DH] = acc[
                    :, h * rows : (h + 1) * rows
                ].T.astype(jnp.bfloat16)
        else:
            acc_ref[j] = acc

    for turn in range(size + 2):

        @pl.when(block >= 0)
        def _():
            if turn < size:
                scores(turn)
            if 0 <= turn - 1 < size:
                softmax(turn - 1)
            if 0 <= turn - 2:
                context(turn - 2)

    if last:
        for k in range(size):
            outs[k][...] = o_buf[pl.ds(pl.multiple_of((member ^ k) * rows, rows), rows), :]


def scratch_of(size, rows, steps):
    keys = len(set(steps) | {0}) * size * rows
    wide = GROUP * rows
    return [
        pltpu.VMEM((size * wide, DH), jnp.bfloat16),
        pltpu.VMEM((keys, DH), jnp.bfloat16),
        pltpu.VMEM((DH, keys), jnp.bfloat16),
        pltpu.VMEM((size * 8, rows), jnp.float32),
        pltpu.VMEM((keys, rows), jnp.float32),
        pltpu.VMEM((2, keys, wide), jnp.float32),
        pltpu.VMEM((2, keys, wide), jnp.bfloat16),
        pltpu.VMEM((size * rows, GROUP * DH), jnp.bfloat16),
        pltpu.VMEM((6, 8, wide), jnp.float32),
    ]


def state_of(size, rows):
    wide = GROUP * rows
    return [
        jax.ShapeDtypeStruct((size * 8, wide), jnp.float32),
        jax.ShapeDtypeStruct((size * 8, wide), jnp.float32),
        jax.ShapeDtypeStruct((size, DH, wide), jnp.float32),
    ]


def layout_of(shards, rows):
    size = 1
    while (2 * size) ** 2 <= shards and 2 * size <= HK:
        size *= 2
    reach = min(WINDOW, rows * shards // 2)
    back = min(-(-(reach - 1) // (size * rows)), shards // size - 1)
    return size, HK // size, back, reach


def local(queries, keys_values, segment_ids, shards):
    rows = queries.shape[0]
    size, chunks, back, reach = layout_of(shards, rows)
    width = GROUP * DH
    me = lax.axis_index("seq")
    place = jnp.stack([me & (size - 1), me >> (size.bit_length() - 1)]).astype(jnp.int32)
    smem = pl.BlockSpec(memory_space=pltpu.SMEM)
    vmem = pl.BlockSpec(memory_space=pltpu.VMEM)
    hbm = pl.BlockSpec(memory_space=pltpu.HBM)
    params = pltpu.CompilerParams(vmem_limit_bytes=48 * 1024 * 1024)
    bf16 = functools.partial(jax.ShapeDtypeStruct, dtype=jnp.bfloat16)

    def call(body, shapes, args, scratch=(), far_in=(), far_out=False):
        return pl.pallas_call(
            body,
            in_specs=[smem if a is place else hbm if n in far_in else vmem for n, a in enumerate(args)],
            out_specs=[hbm if far_out else vmem] * len(shapes),
            out_shape=shapes,
            scratch_shapes=scratch,
            compiler_params=params,
        )(*[pltpu.with_memory_space_constraint(a, pltpu.HBM) if n in far_in else a for n, a in enumerate(args)])

    def swap(x, k):
        return lax.ppermute(x, "seq", [(i, i ^ k) for i in range(shards)]) if k else x

    def onward(x, d):
        return lax.ppermute(x, "seq", [(i, i + size) for i in range((d - 1) * size, shards - size)])

    packed = call(
        functools.partial(pack, size=size, chunks=chunks),
        [bf16((2 * chunks * rows + ID_ROWS, DH))] * size + [bf16((rows, chunks * width))] * size,
        [place, keys_values, segment_ids.reshape(1, rows), queries],
        [pltpu.VMEM((1, rows), jnp.int32), pltpu.SemaphoreType.DMA((1 + 2 * HK + size,))],
        far_in=(1, 2, 3),
    )
    sent, q_sent = packed[:size], packed[size:]
    near = [swap(sent[k], k) for k in range(size)]
    q_parts = [swap(q_sent[k], k) for k in range(size)]
    count = size - 1
    rest_shapes = [bf16((count * (2 * rows + (0 if c else ID_ROWS)), DH)) for c in range(chunks)]
    far_own, far_rest = [sent[0]], []
    if back:
        far_rest.append(call(functools.partial(join, count=count, chunks=chunks, rows=rows), rest_shapes, near[1:]))
    for d in range(1, back + 1):
        far_own.append(onward(far_own[d - 1], d))
        far_rest.append([onward(far_rest[d - 1][c], d) for c in range(chunks)])

    def stage(c, steps, state, first, last):
        args = [place] + q_parts + near
        for d in steps:
            if d:
                args += [far_own[d], far_rest[d][c]] + ([far_rest[d][0]] if c else [])
        args += list(state)
        shapes = [bf16((rows, width))] * size if last else state_of(size, rows)
        scratch = scratch_of(size, rows, steps)
        body = functools.partial(
            attend, chunk=c, size=size, chunks=chunks, rows=rows, reach=reach, steps=steps, first=first, last=last
        )
        return call(body, shapes, args, scratch)

    states = [()] * chunks
    if back:
        states = [stage(c, tuple(range(back)), (), True, False) for c in range(chunks)]
    done = []
    for c in range(chunks):
        result = stage(c, (back,), states[c], not back, True)
        done += [swap(result[k], k) for k in range(size)]
    return call(
        functools.partial(unpack, size=size, chunks=chunks),
        [bf16(queries.shape)],
        [place] + done,
        [pltpu.SemaphoreType.DMA((len(done),))],
        far_out=True,
    )[0]


def solution(mesh):
    shards = mesh.shape["seq"]

    def body(queries, keys_values, segment_ids):
        return local(queries, keys_values, segment_ids, shards)

    return jax.shard_map(
        body,
        mesh=mesh,
        in_specs=(P(("rep", "seq"), None), P(None, ("rep", "seq"), None), P(("rep", "seq"))),
        out_specs=P(("rep", "seq"), None),
        check_vma=False,
    )
```

```python
import functools
import jax
import jax.numpy as jnp
from jax import lax
from jax.experimental import pallas as pl
from jax.experimental.pallas import tpu as pltpu
from jax.sharding import PartitionSpec as P

HQ = 32
HK = 8
DH = 128
WINDOW = 2048

GROUP = HQ // HK
NEG_BIG = -1e30
LOG2E = 1.4426950408889634
ID_ROWS = 16


def early_steps(c, back):
    return 0 if c else back


def pack(place, kv, ids, q, *refs, size, chunks):
    kv_outs, q_outs, (ids_buf, sems) = refs[:size], refs[size : 2 * size], refs[2 * size :]
    rows = kv.shape[1]
    width = q_outs[0].shape[1]
    moves = [(ids, ids_buf)]
    for k in range(size):
        for c in range(chunks):
            start = pl.multiple_of(((place[0] ^ k) * chunks + c) * DH, DH)
            for part in range(2):
                first = (2 * c + part) * rows
                moves.append((kv.at[part, :, pl.ds(start, DH)], kv_outs[k].at[pl.ds(first, rows), :]))
    for k in range(size):
        moves.append((q.at[:, pl.ds(pl.multiple_of((place[0] ^ k) * width, width), width)], q_outs[k]))
    copies = [pltpu.make_async_copy(a, b, sems.at[n]) for n, (a, b) in enumerate(moves)]
    for copy in copies:
        copy.start()
    copies[0].wait()
    tag = jnp.broadcast_to(ids_buf[...].astype(jnp.float32), (ID_ROWS, rows)).astype(jnp.bfloat16)
    for k in range(size):
        kv_outs[k][2 * chunks * rows :, :] = tag
    for copy in copies[1:]:
        copy.wait()


def join(*refs, count, chunks, rows):
    outs = refs[count:]
    for n in range(count):
        for c in range(chunks):
            outs[c][2 * n * rows : 2 * (n + 1) * rows, :] = refs[n][2 * c * rows : 2 * (c + 1) * rows, :]
        outs[0][2 * count * rows + n * ID_ROWS : 2 * count * rows + (n + 1) * ID_ROWS, :] = refs[n][
            2 * chunks * rows :, :
        ]


def join_own(*refs, count, chunk, rows):
    own, rest, out = refs
    out[0 : 2 * rows, :] = own[2 * chunk * rows : 2 * (chunk + 1) * rows, :]
    out[2 * rows : 2 * (count + 1) * rows, :] = rest[0 : 2 * count * rows, :]
    if not chunk:
        tag_at = 2 * (count + 1) * rows
        out[tag_at : tag_at + ID_ROWS, :] = own[own.shape[0] - ID_ROWS :, :]
        out[tag_at + ID_ROWS :, :] = rest[2 * count * rows :, :]


def unpack(place, *refs, chunk, size, chunks):
    out, sems = refs[-2:]
    width = refs[0].shape[1]
    copies = []
    for k in range(size):
        start = pl.multiple_of(((place[0] ^ k) * chunks + chunk) * width, width)
        copies.append(pltpu.make_async_copy(refs[k], out.at[:, pl.ds(start, width)], sems.at[k]))
    for copy in copies:
        copy.start()
    for copy in copies:
        copy.wait()


def attend(place, *refs, chunk, size, chunks, rows, reach, steps, first, last):
    q_refs, near, refs = refs[:size], refs[size : 2 * size], refs[2 * size :]
    far = {}
    for d in steps:
        if d:
            count = (3 if d == 1 else 2) - (0 if chunk else 1)
            far[d] = (refs[0], refs[1 if d == 1 else 0], refs[count - 1])
            refs = refs[count:]
    if not first:
        old_top_ref, old_sum_ref, old_acc_ref = refs[:3]
        refs = refs[3:]
    if last:
        outs, refs = refs[:size], refs[size:]
    else:
        top_ref, sum_ref, acc_ref = refs[:3]
        refs = refs[3:]
    q_buf, k_buf, v_buf, tag_buf, col_buf, s_buf, w_buf, o_buf, stat_buf = refs
    wide = GROUP * rows
    member, block = place[0], place[1]
    tag_at = 2 * chunks * rows
    blocks = sorted(set(steps) | {0}, reverse=True)
    for k in range(size):
        spot = member ^ k
        for d in blocks:
            if d == 0 or (d == 1 and k == 0):
                ref = near[k] if d == 0 else far[d][0]
                start, tag_ref, tag_row = 2 * chunk * rows, ref, tag_at
            else:
                n, count = (k - 1, size - 1) if d == 1 else (k, size)
                ref, tag_ref = far[d][1], far[d][2]
                start, tag_row = 2 * n * rows, 2 * count * rows + n * ID_ROWS
            place_in = blocks.index(d) * size + spot
            tag = tag_ref[tag_row : tag_row + 1, :].astype(jnp.float32)
            if d:
                tag = jnp.where(block >= d, tag, -1.0)
            if d in steps:
                at = pl.ds(pl.multiple_of(place_in * rows, rows), rows)
                k_buf[at, :] = ref[start : start + rows, :]
                v_buf[:, at] = ref[start + rows : start + 2 * rows, :].T
                col_buf[at, :] = jnp.broadcast_to(tag, (rows, rows)).T
            if d == 0:
                tag_buf[pl.ds(pl.multiple_of(spot * 8, 8), 8), :] = jnp.broadcast_to(tag, (8, rows))
        for h in range(GROUP):
            at = pl.ds(pl.multiple_of(spot * wide + h * rows, rows), rows)
            col = (chunk * GROUP + h) * DH
            q_buf[at, :] = q_refs[k][:, col : col + DH]
    ahead = lax.broadcasted_iota(jnp.int32, (rows, rows), 1) - lax.broadcasted_iota(jnp.int32, (rows, rows), 0)
    scale = DH**-0.5 * LOG2E

    def reached(j):
        seen = {}
        for d in steps:
            for n in range(size):
                apart = d * size + j - n
                if apart >= 0 and apart * rows - (rows - 1) < reach:
                    seen[blocks.index(d) * size + n] = apart
        return min(seen) * rows, (max(seen) + 1) * rows, seen

    def scores(j):
        low, high, seen = reached(j)
        q_tag = tag_buf[j * 8 : j * 8 + 1, :]
        s = lax.dot_general(
            k_buf[low:high, :],
            q_buf[j * wide : (j + 1) * wide, :],
            (((1,), (1,)), ((), ())),
            preferred_element_type=jnp.float32,
        )
        top = None
        for u in range(low, high, rows):
            apart = seen[u // rows]
            allowed = col_buf[u : u + rows, :] == q_tag
            if apart == 0:
                allowed = allowed & (ahead >= 0)
            if apart * rows + rows > WINDOW:
                allowed = allowed & (ahead + apart * rows < WINDOW)
            bias = jnp.where(allowed, 0.0, NEG_BIG)
            part = s[u - low : u - low + rows, :] + jnp.concatenate([bias] * GROUP, axis=1)
            s_buf[j % 2, u : u + rows, :] = part
            part = jnp.max(part.reshape(rows // 8, 8, wide), axis=0)
            top = part if top is None else jnp.maximum(top, part)
        stat_buf[j % 2] = top

    def softmax(j):
        low, high, _ = reached(j)
        top = jnp.max(stat_buf[j % 2], axis=0, keepdims=True)
        if not first:
            top = jnp.maximum(top, old_top_ref[j * 8 : j * 8 + 1, :])
        total = None
        for u in range(low, high, rows):
            part = jnp.exp2((s_buf[j % 2, u : u + rows, :] - top) * scale)
            w_buf[j % 2, u : u + rows, :] = part.astype(jnp.bfloat16)
            part = jnp.sum(part.reshape(rows // 8, 8, wide), axis=0)
            total = part if total is None else total + part
        total = jnp.sum(total, axis=0, keepdims=True)
        if not first:
            rescale = jnp.exp2((old_top_ref[j * 8 : j * 8 + 1, :] - top) * scale)
            total = total + old_sum_ref[j * 8 : j * 8 + 1, :] * rescale
            stat_buf[2 + j % 2] = jnp.broadcast_to(rescale, (8, wide))
        if last:
            stat_buf[4 + j % 2] = jnp.broadcast_to(1.0 / total, (8, wide))
        else:
            top_ref[j * 8 : (j + 1) * 8, :] = jnp.broadcast_to(top, (8, wide))
            sum_ref[j * 8 : (j + 1) * 8, :] = jnp.broadcast_to(total, (8, wide))

    def context(j):
        low, high, _ = reached(j)
        acc = jnp.dot(v_buf[:, low:high], w_buf[j % 2, low:high, :], preferred_element_type=jnp.float32)
        if not first:
            acc = acc + old_acc_ref[j] * stat_buf[2 + j % 2, 0:1, :]
        if last:
            acc = acc * stat_buf[4 + j % 2, 0:1, :]
            for h in range(GROUP):
                o_buf[j * rows : (j + 1) * rows, h * DH : (h + 1) * DH] = acc[
                    :, h * rows : (h + 1) * rows
                ].T.astype(jnp.bfloat16)
        else:
            acc_ref[j] = acc

    for turn in range(size + 2):

        @pl.when(block >= 0)
        def _():
            if turn < size:
                scores(turn)
            if 0 <= turn - 1 < size:
                softmax(turn - 1)
            if 0 <= turn - 2:
                context(turn - 2)

    if last:
        for k in range(size):
            outs[k][...] = o_buf[pl.ds(pl.multiple_of((member ^ k) * rows, rows), rows), :]


def scratch_of(size, rows, steps):
    keys = len(set(steps) | {0}) * size * rows
    wide = GROUP * rows
    return [
        pltpu.VMEM((size * wide, DH), jnp.bfloat16),
        pltpu.VMEM((keys, DH), jnp.bfloat16),
        pltpu.VMEM((DH, keys), jnp.bfloat16),
        pltpu.VMEM((size * 8, rows), jnp.float32),
        pltpu.VMEM((keys, rows), jnp.float32),
        pltpu.VMEM((2, keys, wide), jnp.float32),
        pltpu.VMEM((2, keys, wide), jnp.bfloat16),
        pltpu.VMEM((size * rows, GROUP * DH), jnp.bfloat16),
        pltpu.VMEM((6, 8, wide), jnp.float32),
    ]


def state_of(size, rows):
    wide = GROUP * rows
    return [
        jax.ShapeDtypeStruct((size * 8, wide), jnp.float32),
        jax.ShapeDtypeStruct((size * 8, wide), jnp.float32),
        jax.ShapeDtypeStruct((size, DH, wide), jnp.float32),
    ]


def layout_of(shards, rows):
    size = 1
    while (2 * size) ** 2 <= shards and 2 * size <= HK:
        size *= 2
    reach = min(WINDOW, rows * shards // 2)
    back = min(-(-(reach - 1) // (size * rows)), shards // size - 1)
    return size, HK // size, back, reach


def local(queries, keys_values, segment_ids, shards):
    rows = queries.shape[0]
    size, chunks, back, reach = layout_of(shards, rows)
    width = GROUP * DH
    me = lax.axis_index("seq")
    place = jnp.stack([me & (size - 1), me >> (size.bit_length() - 1)]).astype(jnp.int32)
    smem = pl.BlockSpec(memory_space=pltpu.SMEM)
    vmem = pl.BlockSpec(memory_space=pltpu.VMEM)
    hbm = pl.BlockSpec(memory_space=pltpu.HBM)
    params = pltpu.CompilerParams(vmem_limit_bytes=48 * 1024 * 1024)
    bf16 = functools.partial(jax.ShapeDtypeStruct, dtype=jnp.bfloat16)

    def call(body, shapes, args, scratch=(), far_in=(), far_out=False, aliases={}):
        return pl.pallas_call(
            body,
            in_specs=[smem if a is place else hbm if n in far_in else vmem for n, a in enumerate(args)],
            out_specs=[hbm if far_out else vmem] * len(shapes),
            out_shape=shapes,
            scratch_shapes=scratch,
            input_output_aliases=aliases,
            compiler_params=params,
        )(*[pltpu.with_memory_space_constraint(a, pltpu.HBM) if n in far_in else a for n, a in enumerate(args)])

    def swap(x, k):
        return lax.ppermute(x, "seq", [(i, i ^ k) for i in range(shards)]) if k else x

    def onward(x, d):
        return lax.ppermute(x, "seq", [(i, i + size) for i in range((d - 1) * size, shards - size)])

    packed = call(
        functools.partial(pack, size=size, chunks=chunks),
        [bf16((2 * chunks * rows + ID_ROWS, DH))] * size + [bf16((rows, chunks * width))] * size,
        [place, keys_values, segment_ids.reshape(1, rows), queries],
        [pltpu.VMEM((1, rows), jnp.int32), pltpu.SemaphoreType.DMA((1 + 2 * HK + size,))],
        far_in=(1, 2, 3),
    )
    sent, q_sent = packed[:size], packed[size:]
    near = [swap(sent[k], k) for k in range(size)]
    q_parts = [swap(q_sent[k], k) for k in range(size)]
    count = size - 1
    rest_shapes = [bf16((count * (2 * rows + (0 if c else ID_ROWS)), DH)) for c in range(chunks)]
    far = {}
    if back:
        joined = call(functools.partial(join, count=count, chunks=chunks, rows=rows), rest_shapes, near[1:])
        own = onward(sent[0], 1)
        rest = [onward(joined[c], 1) for c in range(chunks)]
        far[1] = [[own, rest[c]] for c in range(chunks)]
    for d in range(2, back + 1):
        far[d] = []
        for c in range(chunks):
            if d == 2:
                shape = bf16((size * (2 * rows + (0 if c else ID_ROWS)), DH))
                body = functools.partial(join_own, count=count, chunk=c, rows=rows)
                last = call(body, [shape], [own, rest[c]])[0]
            else:
                last = far[d - 1][c][0]
            far[d].append([onward(last, d)])

    def stage(c, steps, state, first, last):
        args = [place] + q_parts + near
        for d in steps:
            if d:
                args += far[d][c] + (far[d][0][-1:] if c else [])
        args += list(state)
        shapes = [bf16((rows, width))] * size if last else state_of(size, rows)
        scratch = scratch_of(size, rows, steps)
        body = functools.partial(
            attend, chunk=c, size=size, chunks=chunks, rows=rows, reach=reach, steps=steps, first=first, last=last
        )
        return call(body, shapes, args, scratch)

    out = None
    for c in range(chunks):
        state, steps = (), tuple(range(back + 1))
        early = early_steps(c, back)
        if early:
            state = stage(c, steps[:early], (), True, False)
            steps = steps[early:]
        result = stage(c, steps, state, not state, True)
        done = [swap(result[k], k) for k in range(size)]
        args = [place] + done + ([out] if c else [])
        out = call(
            functools.partial(unpack, chunk=c, size=size, chunks=chunks),
            [bf16(queries.shape)],
            args,
            [pltpu.SemaphoreType.DMA((size,))],
            far_in=(1 + size,) if c else (),
            far_out=True,
            aliases={1 + size: 0} if c else {},
        )[0]
    return out


def solution(mesh):
    shards = mesh.shape["seq"]

    def body(queries, keys_values, segment_ids):
        return local(queries, keys_values, segment_ids, shards)

    return jax.shard_map(
        body,
        mesh=mesh,
        in_specs=(P(("rep", "seq"), None), P(None, ("rep", "seq"), None), P(("rep", "seq"))),
        out_specs=P(("rep", "seq"), None),
        check_vma=False,
    )
```

```python
import functools
import jax
import jax.numpy as jnp
from jax import lax
from jax.experimental import pallas as pl
from jax.experimental.pallas import tpu as pltpu
from jax.sharding import PartitionSpec as P

HQ = 32
HK = 8
DH = 128
WINDOW = 2048

GROUP = HQ // HK
NEG_BIG = -1e30
LOG2E = 1.4426950408889634
ID_ROWS = 16


def early_steps(c, back):
    return 0 if c else back


def pack(place, kv, ids, q, *refs, size, chunks):
    kv_outs, q_outs, (ids_buf, sems) = refs[:size], refs[size : 2 * size], refs[2 * size :]
    rows = kv.shape[1]
    width = q_outs[0].shape[1]
    moves = [(ids, ids_buf)]
    for k in range(size):
        for c in range(chunks):
            start = pl.multiple_of(((place[0] ^ k) * chunks + c) * DH, DH)
            for part in range(2):
                first = (2 * c + part) * rows
                moves.append((kv.at[part, :, pl.ds(start, DH)], kv_outs[k].at[pl.ds(first, rows), :]))
    for k in range(size):
        moves.append((q.at[:, pl.ds(pl.multiple_of((place[0] ^ k) * width, width), width)], q_outs[k]))
    copies = [pltpu.make_async_copy(a, b, sems.at[n]) for n, (a, b) in enumerate(moves)]
    for copy in copies:
        copy.start()
    copies[0].wait()
    tag = jnp.broadcast_to(ids_buf[...].astype(jnp.float32), (ID_ROWS, rows)).astype(jnp.bfloat16)
    for k in range(size):
        kv_outs[k][2 * chunks * rows :, :] = tag
    for copy in copies[1:]:
        copy.wait()


def join(*refs, count, chunks, rows):
    outs = refs[count:]
    for n in range(count):
        for c in range(chunks):
            outs[c][2 * n * rows : 2 * (n + 1) * rows, :] = refs[n][2 * c * rows : 2 * (c + 1) * rows, :]
        outs[0][2 * count * rows + n * ID_ROWS : 2 * count * rows + (n + 1) * ID_ROWS, :] = refs[n][
            2 * chunks * rows :, :
        ]


def join_own(*refs, count, chunk, rows):
    own, rest, out = refs
    out[0 : 2 * rows, :] = own[2 * chunk * rows : 2 * (chunk + 1) * rows, :]
    out[2 * rows : 2 * (count + 1) * rows, :] = rest[0 : 2 * count * rows, :]
    if not chunk:
        tag_at = 2 * (count + 1) * rows
        out[tag_at : tag_at + ID_ROWS, :] = own[own.shape[0] - ID_ROWS :, :]
        out[tag_at + ID_ROWS :, :] = rest[2 * count * rows :, :]


def unpack(place, *refs, chunk, size, chunks):
    out, sems = refs[-2:]
    width = refs[0].shape[1]
    copies = []
    for k in range(size):
        start = pl.multiple_of(((place[0] ^ k) * chunks + chunk) * width, width)
        copies.append(pltpu.make_async_copy(refs[k], out.at[:, pl.ds(start, width)], sems.at[k]))
    for copy in copies:
        copy.start()
    for copy in copies:
        copy.wait()


def attend(place, *refs, chunk, size, chunks, rows, reach, steps, first, last):
    q_refs, near, refs = refs[:size], refs[size : 2 * size], refs[2 * size :]
    far = {}
    for d in steps:
        if d:
            count = (3 if d == 1 else 2) - (0 if chunk else 1)
            far[d] = (refs[0], refs[1 if d == 1 else 0], refs[count - 1])
            refs = refs[count:]
    if not first:
        old_top_ref, old_sum_ref, old_acc_ref = refs[:3]
        refs = refs[3:]
    if last:
        outs, refs = refs[:size], refs[size:]
    else:
        top_ref, sum_ref, acc_ref = refs[:3]
        refs = refs[3:]
    q_buf, k_buf, v_buf, tag_buf, col_buf, s_buf, w_buf, o_buf, stat_buf = refs
    wide = GROUP * rows
    member, block = place[0], place[1]
    tag_at = 2 * chunks * rows
    blocks = sorted(set(steps) | {0}, reverse=True)
    for k in range(size):
        spot = member ^ k
        for d in blocks:
            if d == 0 or (d == 1 and k == 0):
                ref = near[k] if d == 0 else far[d][0]
                start, tag_ref, tag_row = 2 * chunk * rows, ref, tag_at
            else:
                n, count = (k - 1, size - 1) if d == 1 else (k, size)
                ref, tag_ref = far[d][1], far[d][2]
                start, tag_row = 2 * n * rows, 2 * count * rows + n * ID_ROWS
            place_in = blocks.index(d) * size + spot
            tag = tag_ref[tag_row : tag_row + 1, :].astype(jnp.float32)
            if d:
                tag = jnp.where(block >= d, tag, -1.0)
            if d in steps:
                at = pl.ds(pl.multiple_of(place_in * rows, rows), rows)
                k_buf[at, :] = ref[start : start + rows, :]
                v_buf[:, at] = ref[start + rows : start + 2 * rows, :].T
                col_buf[at, :] = jnp.broadcast_to(tag, (rows, rows)).T
            if d == 0:
                tag_buf[pl.ds(pl.multiple_of(spot * 8, 8), 8), :] = jnp.broadcast_to(tag, (8, rows))
        for h in range(GROUP):
            at = pl.ds(pl.multiple_of(spot * wide + h * rows, rows), rows)
            col = (chunk * GROUP + h) * DH
            q_buf[at, :] = q_refs[k][:, col : col + DH]
    ahead = lax.broadcasted_iota(jnp.int32, (rows, rows), 1) - lax.broadcasted_iota(jnp.int32, (rows, rows), 0)
    scale = DH**-0.5 * LOG2E

    def reached(j):
        seen = {}
        for d in steps:
            for n in range(size):
                apart = d * size + j - n
                if apart >= 0 and apart * rows - (rows - 1) < reach:
                    seen[blocks.index(d) * size + n] = apart
        return min(seen) * rows, (max(seen) + 1) * rows, seen

    def scores(j):
        low, high, seen = reached(j)
        q_tag = tag_buf[j * 8 : j * 8 + 1, :]
        s = lax.dot_general(
            k_buf[low:high, :],
            q_buf[j * wide : (j + 1) * wide, :],
            (((1,), (1,)), ((), ())),
            preferred_element_type=jnp.float32,
        )
        top = None
        for u in range(low, high, rows):
            apart = seen[u // rows]
            allowed = col_buf[u : u + rows, :] == q_tag
            if apart == 0:
                allowed = allowed & (ahead >= 0)
            if apart * rows + rows > WINDOW:
                allowed = allowed & (ahead + apart * rows < WINDOW)
            bias = jnp.where(allowed, 0.0, NEG_BIG)
            part = s[u - low : u - low + rows, :] + jnp.concatenate([bias] * GROUP, axis=1)
            s_buf[j % 2, u : u + rows, :] = part
            part = jnp.max(part.reshape(rows // 8, 8, wide), axis=0)
            top = part if top is None else jnp.maximum(top, part)
        stat_buf[j % 2] = top

    def softmax(j):
        low, high, _ = reached(j)
        top = jnp.max(stat_buf[j % 2], axis=0, keepdims=True)
        if not first:
            top = jnp.maximum(top, old_top_ref[j * 8 : j * 8 + 1, :])
        total = None
        for u in range(low, high, rows):
            part = jnp.exp2((s_buf[j % 2, u : u + rows, :] - top) * scale)
            w_buf[j % 2, u : u + rows, :] = part.astype(jnp.bfloat16)
            part = jnp.sum(part.reshape(rows // 8, 8, wide), axis=0)
            total = part if total is None else total + part
        total = jnp.sum(total, axis=0, keepdims=True)
        if not first:
            rescale = jnp.exp2((old_top_ref[j * 8 : j * 8 + 1, :] - top) * scale)
            total = total + old_sum_ref[j * 8 : j * 8 + 1, :] * rescale
            stat_buf[2 + j % 2] = jnp.broadcast_to(rescale, (8, wide))
        if last:
            stat_buf[4 + j % 2] = jnp.broadcast_to(1.0 / total, (8, wide))
        else:
            top_ref[j * 8 : (j + 1) * 8, :] = jnp.broadcast_to(top, (8, wide))
            sum_ref[j * 8 : (j + 1) * 8, :] = jnp.broadcast_to(total, (8, wide))

    def context(j):
        low, high, _ = reached(j)
        acc = jnp.dot(v_buf[:, low:high], w_buf[j % 2, low:high, :], preferred_element_type=jnp.float32)
        if not first:
            acc = acc + old_acc_ref[j] * stat_buf[2 + j % 2, 0:1, :]
        if last:
            acc = acc * stat_buf[4 + j % 2, 0:1, :]
            for h in range(GROUP):
                o_buf[j * rows : (j + 1) * rows, h * DH : (h + 1) * DH] = acc[
                    :, h * rows : (h + 1) * rows
                ].T.astype(jnp.bfloat16)
        else:
            acc_ref[j] = acc

    for turn in range(size + 2):

        @pl.when(block >= 0)
        def _():
            if turn < size:
                scores(turn)
            if 0 <= turn - 1 < size:
                softmax(turn - 1)
            if 0 <= turn - 2:
                context(turn - 2)

    if last:
        for k in range(size):
            outs[k][...] = o_buf[pl.ds(pl.multiple_of((member ^ k) * rows, rows), rows), :]


def scratch_of(size, rows, steps):
    keys = len(set(steps) | {0}) * size * rows
    wide = GROUP * rows
    return [
        pltpu.VMEM((size * wide, DH), jnp.bfloat16),
        pltpu.VMEM((keys, DH), jnp.bfloat16),
        pltpu.VMEM((DH, keys), jnp.bfloat16),
        pltpu.VMEM((size * 8, rows), jnp.float32),
        pltpu.VMEM((keys, rows), jnp.float32),
        pltpu.VMEM((2, keys, wide), jnp.float32),
        pltpu.VMEM((2, keys, wide), jnp.bfloat16),
        pltpu.VMEM((size * rows, GROUP * DH), jnp.bfloat16),
        pltpu.VMEM((6, 8, wide), jnp.float32),
    ]


def state_of(size, rows):
    wide = GROUP * rows
    return [
        jax.ShapeDtypeStruct((size * 8, wide), jnp.float32),
        jax.ShapeDtypeStruct((size * 8, wide), jnp.float32),
        jax.ShapeDtypeStruct((size, DH, wide), jnp.float32),
    ]


def layout_of(shards, rows):
    size = 1
    while (2 * size) ** 2 <= shards and 2 * size <= HK:
        size *= 2
    reach = min(WINDOW, rows * shards // 2)
    back = min(-(-(reach - 1) // (size * rows)), shards // size - 1)
    return size, HK // size, back, reach


def local(queries, keys_values, segment_ids, shards):
    rows = queries.shape[0]
    size, chunks, back, reach = layout_of(shards, rows)
    width = GROUP * DH
    me = lax.axis_index("seq")
    place = jnp.stack([me & (size - 1), me >> (size.bit_length() - 1)]).astype(jnp.int32)
    smem = pl.BlockSpec(memory_space=pltpu.SMEM)
    vmem = pl.BlockSpec(memory_space=pltpu.VMEM)
    hbm = pl.BlockSpec(memory_space=pltpu.HBM)
    params = pltpu.CompilerParams(vmem_limit_bytes=48 * 1024 * 1024)
    bf16 = functools.partial(jax.ShapeDtypeStruct, dtype=jnp.bfloat16)

    def call(body, shapes, args, scratch=(), far_in=(), far_out=False, aliases={}):
        return pl.pallas_call(
            body,
            in_specs=[smem if a is place else hbm if n in far_in else vmem for n, a in enumerate(args)],
            out_specs=[hbm if far_out else vmem] * len(shapes),
            out_shape=shapes,
            scratch_shapes=scratch,
            input_output_aliases=aliases,
            compiler_params=params,
        )(*[pltpu.with_memory_space_constraint(a, pltpu.HBM) if n in far_in else a for n, a in enumerate(args)])

    def swap(x, k):
        return lax.ppermute(x, "seq", [(i, i ^ k) for i in range(shards)]) if k else x

    def onward(x, d):
        pairs = [(i, (i + size) % shards) for i in range(shards)]
        if d > 1:
            pairs = pairs[(d - 1) * size : shards - size]
        return lax.ppermute(x, "seq", pairs)

    packed = call(
        functools.partial(pack, size=size, chunks=chunks),
        [bf16((2 * chunks * rows + ID_ROWS, DH))] * size + [bf16((rows, chunks * width))] * size,
        [place, keys_values, segment_ids.reshape(1, rows), queries],
        [pltpu.VMEM((1, rows), jnp.int32), pltpu.SemaphoreType.DMA((1 + 2 * HK + size,))],
        far_in=(1, 2, 3),
    )
    sent, q_sent = packed[:size], packed[size:]
    near = [swap(sent[k], k) for k in range(size)]
    q_parts = [swap(q_sent[k], k) for k in range(size)]
    count = size - 1
    rest_shapes = [bf16((count * (2 * rows + (0 if c else ID_ROWS)), DH)) for c in range(chunks)]
    far = {}
    if back:
        joined = call(functools.partial(join, count=count, chunks=chunks, rows=rows), rest_shapes, near[1:])
        own = onward(sent[0], 1)
        rest = [onward(joined[c], 1) for c in range(chunks)]
        far[1] = [[own, rest[c]] for c in range(chunks)]
    for d in range(2, back + 1):
        far[d] = []
        for c in range(chunks):
            if d == 2:
                shape = bf16((size * (2 * rows + (0 if c else ID_ROWS)), DH))
                body = functools.partial(join_own, count=count, chunk=c, rows=rows)
                last = call(body, [shape], [own, rest[c]])[0]
            else:
                last = far[d - 1][c][0]
            far[d].append([onward(last, d)])

    def stage(c, steps, state, first, last):
        args = [place] + q_parts + near
        for d in steps:
            if d:
                args += far[d][c] + (far[d][0][-1:] if c else [])
        args += list(state)
        shapes = [bf16((rows, width))] * size if last else state_of(size, rows)
        scratch = scratch_of(size, rows, steps)
        body = functools.partial(
            attend, chunk=c, size=size, chunks=chunks, rows=rows, reach=reach, steps=steps, first=first, last=last
        )
        return call(body, shapes, args, scratch)

    out = None
    for c in range(chunks):
        state, steps = (), tuple(range(back + 1))
        early = early_steps(c, back)
        if early:
            state = stage(c, steps[:early], (), True, False)
            steps = steps[early:]
        result = stage(c, steps, state, not state, True)
        done = [swap(result[k], k) for k in range(size)]
        args = [place] + done + ([out] if c else [])
        out = call(
            functools.partial(unpack, chunk=c, size=size, chunks=chunks),
            [bf16(queries.shape)],
            args,
            [pltpu.SemaphoreType.DMA((size,))],
            far_in=(1 + size,) if c else (),
            far_out=True,
            aliases={1 + size: 0} if c else {},
        )[0]
    return out


def solution(mesh):
    shards = mesh.shape["seq"]

    def body(queries, keys_values, segment_ids):
        return local(queries, keys_values, segment_ids, shards)

    return jax.shard_map(
        body,
        mesh=mesh,
        in_specs=(P(("rep", "seq"), None), P(None, ("rep", "seq"), None), P(("rep", "seq"))),
        out_specs=P(("rep", "seq"), None),
        check_vma=False,
    )
```

```python
import functools
import jax
import jax.numpy as jnp
from jax import lax
from jax.experimental import pallas as pl
from jax.experimental.pallas import tpu as pltpu
from jax.sharding import PartitionSpec as P

HQ = 32
HK = 8
DH = 128
WINDOW = 2048

GROUP = HQ // HK
NEG_BIG = -1e30
LOG2E = 1.4426950408889634
ID_ROWS = 16


def early_steps(c, back):
    return 0 if c else back


def pack_kv(place, kv, ids, *refs, size, chunks):
    outs, (ids_buf, sems) = refs[:size], refs[size:]
    rows = kv.shape[1]
    moves = [(ids, ids_buf)]
    for k in range(size):
        for c in range(chunks):
            start = pl.multiple_of(((place[0] ^ k) * chunks + c) * DH, DH)
            for part in range(2):
                first = (2 * c + part) * rows
                moves.append((kv.at[part, :, pl.ds(start, DH)], outs[k].at[pl.ds(first, rows), :]))
    copies = [pltpu.make_async_copy(a, b, sems.at[n]) for n, (a, b) in enumerate(moves)]
    for copy in copies:
        copy.start()
    copies[0].wait()
    tag = jnp.broadcast_to(ids_buf[...].astype(jnp.float32), (ID_ROWS, rows)).astype(jnp.bfloat16)
    for k in range(size):
        outs[k][2 * chunks * rows :, :] = tag
    for copy in copies[1:]:
        copy.wait()


def pack_q(place, q, *refs, size):
    outs, sems = refs[:size], refs[size]
    width = outs[0].shape[1]
    copies = []
    for k in range(size):
        start = pl.multiple_of((place[0] ^ k) * width, width)
        copies.append(pltpu.make_async_copy(q.at[:, pl.ds(start, width)], outs[k], sems.at[k]))
    for copy in copies:
        copy.start()
    for copy in copies:
        copy.wait()


def join(*refs, count, chunks, rows):
    outs = refs[count:]
    for n in range(count):
        for c in range(chunks):
            outs[c][2 * n * rows : 2 * (n + 1) * rows, :] = refs[n][2 * c * rows : 2 * (c + 1) * rows, :]
        outs[0][2 * count * rows + n * ID_ROWS : 2 * count * rows + (n + 1) * ID_ROWS, :] = refs[n][
            2 * chunks * rows :, :
        ]


def join_own(*refs, count, chunk, rows):
    own, rest, out = refs
    out[0 : 2 * rows, :] = own[2 * chunk * rows : 2 * (chunk + 1) * rows, :]
    out[2 * rows : 2 * (count + 1) * rows, :] = rest[0 : 2 * count * rows, :]
    if not chunk:
        tag_at = 2 * (count + 1) * rows
        out[tag_at : tag_at + ID_ROWS, :] = own[own.shape[0] - ID_ROWS :, :]
        out[tag_at + ID_ROWS :, :] = rest[2 * count * rows :, :]


def unpack(place, *refs, chunk, size, chunks):
    out, sems = refs[-2:]
    width = refs[0].shape[1]
    copies = []
    for k in range(size):
        start = pl.multiple_of(((place[0] ^ k) * chunks + chunk) * width, width)
        copies.append(pltpu.make_async_copy(refs[k], out.at[:, pl.ds(start, width)], sems.at[k]))
    for copy in copies:
        copy.start()
    for copy in copies:
        copy.wait()


def attend(place, *refs, chunk, size, chunks, rows, reach, steps, first, last):
    q_refs, near, refs = refs[:size], refs[size : 2 * size], refs[2 * size :]
    far = {}
    for d in steps:
        if d:
            count = (3 if d == 1 else 2) - (0 if chunk else 1)
            far[d] = (refs[0], refs[1 if d == 1 else 0], refs[count - 1])
            refs = refs[count:]
    if not first:
        old_top_ref, old_sum_ref, old_acc_ref = refs[:3]
        refs = refs[3:]
    if last:
        outs, refs = refs[:size], refs[size:]
    else:
        top_ref, sum_ref, acc_ref = refs[:3]
        refs = refs[3:]
    q_buf, k_buf, v_buf, tag_buf, col_buf, s_buf, w_buf, o_buf, stat_buf = refs
    wide = GROUP * rows
    member, block = place[0], place[1]
    tag_at = 2 * chunks * rows
    blocks = sorted(set(steps) | {0}, reverse=True)
    for k in range(size):
        spot = member ^ k
        for d in blocks:
            if d == 0 or (d == 1 and k == 0):
                ref = near[k] if d == 0 else far[d][0]
                start, tag_ref, tag_row = 2 * chunk * rows, ref, tag_at
            else:
                n, count = (k - 1, size - 1) if d == 1 else (k, size)
                ref, tag_ref = far[d][1], far[d][2]
                start, tag_row = 2 * n * rows, 2 * count * rows + n * ID_ROWS
            place_in = blocks.index(d) * size + spot
            tag = tag_ref[tag_row : tag_row + 1, :].astype(jnp.float32)
            if d:
                tag = jnp.where(block >= d, tag, -1.0)
            if d in steps:
                at = pl.ds(pl.multiple_of(place_in * rows, rows), rows)
                k_buf[at, :] = ref[start : start + rows, :]
                v_buf[:, at] = ref[start + rows : start + 2 * rows, :].T
                col_buf[at, :] = jnp.broadcast_to(tag, (rows, rows)).T
            if d == 0:
                tag_buf[pl.ds(pl.multiple_of(spot * 8, 8), 8), :] = jnp.broadcast_to(tag, (8, rows))
        for h in range(GROUP):
            at = pl.ds(pl.multiple_of(spot * wide + h * rows, rows), rows)
            col = (chunk * GROUP + h) * DH
            q_buf[at, :] = q_refs[k][:, col : col + DH]
    ahead = lax.broadcasted_iota(jnp.int32, (rows, rows), 1) - lax.broadcasted_iota(jnp.int32, (rows, rows), 0)
    scale = DH**-0.5 * LOG2E

    def reached(j):
        seen = {}
        for d in steps:
            for n in range(size):
                apart = d * size + j - n
                if apart >= 0 and apart * rows - (rows - 1) < reach:
                    seen[blocks.index(d) * size + n] = apart
        return min(seen) * rows, (max(seen) + 1) * rows, seen

    def scores(j):
        low, high, seen = reached(j)
        q_tag = tag_buf[j * 8 : j * 8 + 1, :]
        s = lax.dot_general(
            k_buf[low:high, :],
            q_buf[j * wide : (j + 1) * wide, :],
            (((1,), (1,)), ((), ())),
            preferred_element_type=jnp.float32,
        )
        top = None
        for u in range(low, high, rows):
            apart = seen[u // rows]
            allowed = col_buf[u : u + rows, :] == q_tag
            if apart == 0:
                allowed = allowed & (ahead >= 0)
            if apart * rows + rows > WINDOW:
                allowed = allowed & (ahead + apart * rows < WINDOW)
            bias = jnp.where(allowed, 0.0, NEG_BIG)
            part = s[u - low : u - low + rows, :] + jnp.concatenate([bias] * GROUP, axis=1)
            s_buf[j % 2, u : u + rows, :] = part
            part = jnp.max(part.reshape(rows // 8, 8, wide), axis=0)
            top = part if top is None else jnp.maximum(top, part)
        stat_buf[j % 2] = top

    def softmax(j):
        low, high, _ = reached(j)
        top = jnp.max(stat_buf[j % 2], axis=0, keepdims=True)
        if not first:
            top = jnp.maximum(top, old_top_ref[j * 8 : j * 8 + 1, :])
        total = None
        for u in range(low, high, rows):
            part = jnp.exp2((s_buf[j % 2, u : u + rows, :] - top) * scale)
            w_buf[j % 2, u : u + rows, :] = part.astype(jnp.bfloat16)
            part = jnp.sum(part.reshape(rows // 8, 8, wide), axis=0)
            total = part if total is None else total + part
        total = jnp.sum(total, axis=0, keepdims=True)
        if not first:
            rescale = jnp.exp2((old_top_ref[j * 8 : j * 8 + 1, :] - top) * scale)
            total = total + old_sum_ref[j * 8 : j * 8 + 1, :] * rescale
            stat_buf[2 + j % 2] = jnp.broadcast_to(rescale, (8, wide))
        if last:
            stat_buf[4 + j % 2] = jnp.broadcast_to(1.0 / total, (8, wide))
        else:
            top_ref[j * 8 : (j + 1) * 8, :] = jnp.broadcast_to(top, (8, wide))
            sum_ref[j * 8 : (j + 1) * 8, :] = jnp.broadcast_to(total, (8, wide))

    def context(j):
        low, high, _ = reached(j)
        acc = jnp.dot(v_buf[:, low:high], w_buf[j % 2, low:high, :], preferred_element_type=jnp.float32)
        if not first:
            acc = acc + old_acc_ref[j] * stat_buf[2 + j % 2, 0:1, :]
        if last:
            acc = acc * stat_buf[4 + j % 2, 0:1, :]
            for h in range(GROUP):
                o_buf[j * rows : (j + 1) * rows, h * DH : (h + 1) * DH] = acc[
                    :, h * rows : (h + 1) * rows
                ].T.astype(jnp.bfloat16)
        else:
            acc_ref[j] = acc

    for turn in range(size + 2):

        @pl.when(block >= 0)
        def _():
            if turn < size:
                scores(turn)
            if 0 <= turn - 1 < size:
                softmax(turn - 1)
            if 0 <= turn - 2:
                context(turn - 2)

    if last:
        for k in range(size):
            outs[k][...] = o_buf[pl.ds(pl.multiple_of((member ^ k) * rows, rows), rows), :]


def scratch_of(size, rows, steps):
    keys = len(set(steps) | {0}) * size * rows
    wide = GROUP * rows
    return [
        pltpu.VMEM((size * wide, DH), jnp.bfloat16),
        pltpu.VMEM((keys, DH), jnp.bfloat16),
        pltpu.VMEM((DH, keys), jnp.bfloat16),
        pltpu.VMEM((size * 8, rows), jnp.float32),
        pltpu.VMEM((keys, rows), jnp.float32),
        pltpu.VMEM((2, keys, wide), jnp.float32),
        pltpu.VMEM((2, keys, wide), jnp.bfloat16),
        pltpu.VMEM((size * rows, GROUP * DH), jnp.bfloat16),
        pltpu.VMEM((6, 8, wide), jnp.float32),
    ]


def state_of(size, rows):
    wide = GROUP * rows
    return [
        jax.ShapeDtypeStruct((size * 8, wide), jnp.float32),
        jax.ShapeDtypeStruct((size * 8, wide), jnp.float32),
        jax.ShapeDtypeStruct((size, DH, wide), jnp.float32),
    ]


def layout_of(shards, rows):
    size = 1
    while (2 * size) ** 2 <= shards and 2 * size <= HK:
        size *= 2
    reach = min(WINDOW, rows * shards // 2)
    back = min(-(-(reach - 1) // (size * rows)), shards // size - 1)
    return size, HK // size, back, reach


def local(queries, keys_values, segment_ids, shards):
    rows = queries.shape[0]
    size, chunks, back, reach = layout_of(shards, rows)
    width = GROUP * DH
    me = lax.axis_index("seq")
    place = jnp.stack([me & (size - 1), me >> (size.bit_length() - 1)]).astype(jnp.int32)
    smem = pl.BlockSpec(memory_space=pltpu.SMEM)
    vmem = pl.BlockSpec(memory_space=pltpu.VMEM)
    hbm = pl.BlockSpec(memory_space=pltpu.HBM)
    params = pltpu.CompilerParams(vmem_limit_bytes=48 * 1024 * 1024)
    bf16 = functools.partial(jax.ShapeDtypeStruct, dtype=jnp.bfloat16)

    def call(body, shapes, args, scratch=(), far_in=(), far_out=False, aliases={}):
        return pl.pallas_call(
            body,
            in_specs=[smem if a is place else hbm if n in far_in else vmem for n, a in enumerate(args)],
            out_specs=[hbm if far_out else vmem] * len(shapes),
            out_shape=shapes,
            scratch_shapes=scratch,
            input_output_aliases=aliases,
            compiler_params=params,
        )(*[pltpu.with_memory_space_constraint(a, pltpu.HBM) if n in far_in else a for n, a in enumerate(args)])

    def swap(x, k):
        return lax.ppermute(x, "seq", [(i, i ^ k) for i in range(shards)]) if k else x

    def onward(x, d):
        pairs = [(i, (i + size) % shards) for i in range(shards)]
        if d > 1:
            pairs = pairs[(d - 1) * size : shards - size]
        return lax.ppermute(x, "seq", pairs)

    sent = call(
        functools.partial(pack_kv, size=size, chunks=chunks),
        [bf16((2 * chunks * rows + ID_ROWS, DH))] * size,
        [place, keys_values, segment_ids.reshape(1, rows)],
        [pltpu.VMEM((1, rows), jnp.int32), pltpu.SemaphoreType.DMA((1 + 2 * HK,))],
        far_in=(1, 2),
    )
    q_sent = call(
        functools.partial(pack_q, size=size),
        [bf16((rows, chunks * width))] * size,
        [place, queries],
        [pltpu.SemaphoreType.DMA((size,))],
        far_in=(1,),
    )
    near = [swap(sent[k], k) for k in range(size)]
    q_parts = [swap(q_sent[k], k) for k in range(size)]
    count = size - 1
    rest_shapes = [bf16((count * (2 * rows + (0 if c else ID_ROWS)), DH)) for c in range(chunks)]
    far = {}
    if back:
        joined = call(functools.partial(join, count=count, chunks=chunks, rows=rows), rest_shapes, near[1:])
        own = onward(sent[0], 1)
        rest = [onward(joined[c], 1) for c in range(chunks)]
        far[1] = [[own, rest[c]] for c in range(chunks)]
    for d in range(2, back + 1):
        far[d] = []
        for c in range(chunks):
            if d == 2:
                shape = bf16((size * (2 * rows + (0 if c else ID_ROWS)), DH))
                body = functools.partial(join_own, count=count, chunk=c, rows=rows)
                last = call(body, [shape], [own, rest[c]])[0]
            else:
                last = far[d - 1][c][0]
            far[d].append([onward(last, d)])

    def stage(c, steps, state, first, last):
        args = [place] + q_parts + near
        for d in steps:
            if d:
                args += far[d][c] + (far[d][0][-1:] if c else [])
        args += list(state)
        shapes = [bf16((rows, width))] * size if last else state_of(size, rows)
        scratch = scratch_of(size, rows, steps)
        body = functools.partial(
            attend, chunk=c, size=size, chunks=chunks, rows=rows, reach=reach, steps=steps, first=first, last=last
        )
        return call(body, shapes, args, scratch)

    out = None
    for c in range(chunks):
        state, steps = (), tuple(range(back + 1))
        early = early_steps(c, back)
        if early:
            state = stage(c, steps[:early], (), True, False)
            steps = steps[early:]
        result = stage(c, steps, state, not state, True)
        done = [swap(result[k], k) for k in range(size)]
        args = [place] + done + ([out] if c else [])
        out = call(
            functools.partial(unpack, chunk=c, size=size, chunks=chunks),
            [bf16(queries.shape)],
            args,
            [pltpu.SemaphoreType.DMA((size,))],
            far_in=(1 + size,) if c else (),
            far_out=True,
            aliases={1 + size: 0} if c else {},
        )[0]
    return out


def solution(mesh):
    shards = mesh.shape["seq"]

    def body(queries, keys_values, segment_ids):
        return local(queries, keys_values, segment_ids, shards)

    return jax.shard_map(
        body,
        mesh=mesh,
        in_specs=(P(("rep", "seq"), None), P(None, ("rep", "seq"), None), P(("rep", "seq"))),
        out_specs=P(("rep", "seq"), None),
        check_vma=False,
    )
```
